256 devices in a mesh: cells: 16 (over y, z_hi), grp: 16 (over x, z_lo, core).
Axes of the slice: x: 4, y: 4, z: 8 (z_hi: 4, z_lo: 2; z = z_hi * 2 + z_lo), core: 2. Of those that a mesh axis runs over, the one named last changes fastest.
Arguments:
- coeffs: bfloat16 [4096, 6144], P(('cells', 'grp')), may hold values from -6 to 6
- neighbours: int32 [4096, 32], P(('cells', 'grp')), may hold values from 0 to 47
- counts: int32 [4096], P(('cells', 'grp')), may hold values from 8 to 32
- boxes: int32 [4096], P(('cells', 'grp')), may hold values from 0 to 31
- axial: bfloat16 [4096, 32, 96], P(('cells', 'grp')), may hold values from -1 to 1
- rotations: bfloat16 [32, 96, 96], replicated, may hold values from -0.625 to 0.625
- out_map: bfloat16 [96, 96], replicated, may hold values from -0.625 to 0.625
- coupling: bfloat16 [512, 512], replicated, may hold values from -1 to 1, as said below
- in_map: bfloat16 [96, 96], replicated, may hold values from -0.21875 to 0.21875
- tmat: float32 [4096, 96], P(('cells', 'grp')), may hold values from -0.5 to 0.5
Outputs:
- product: bfloat16 [4096, 6144], P(('cells', 'grp'))
The draws below stay inside these ranges and needn't reach their ends.
Inputs may be any that keep to these rules, and one draw needn't show every extreme that they name: Entries of coupling are zero on the diagonal.
All inputs are finite; a program needn't handle non-finite values.
Results may differ from the reference program's by a relative error of at most 0.0043.
Values may be sent and summed in bfloat16 or wider, within the bound.
No kernel may reach another device: no remote copies, remote signals or barrier semaphores. Data moves between devices by JAX's collectives and lax.ppermute only.
A program may use at most 64 MiB of HBM per device.

```python
import jax
import jax.numpy as jnp
from jax import lax

C = 96
P_SIZE = 64
K = 32
SD = 16
NBG = 2
NBC = 32
NBOX = 512
BOX_SPH = 8
S = 4096
N_CELLS = 16
N_GRP = 16


def draw_coupling(key, part):
    values = jax.random.normal(key, (NBOX, NBOX), jnp.float32) * (2.0 / NBOX ** 0.5)
    values = jnp.clip(values, -1.0, 1.0)
    rows = jnp.arange(NBOX, dtype=jnp.int32)
    offdiag = (rows[:, None] != rows[None, :]).astype(jnp.float32)
    return (values * offdiag).astype(jnp.bfloat16)


def place_ends(entries, rng, least, largest):
    index_at = [jax.random.randint(jax.random.fold_in(rng, axis), (), 0, length) for axis, length in enumerate(entries.shape)]
    longest = entries.shape.index(max(entries.shape))
    next_to = index_at[:longest] + [(index_at[longest] + 1) % entries.shape[longest]] + index_at[longest + 1:]
    return entries.at[tuple(index_at)].set(least).at[tuple(next_to)].set(largest)


def levels(rng, shape, pieces, smallest, largest):
    factor_of, own = 1.0, jax.random.fold_in(rng, 6)
    for axis_at, parts in pieces:
        heights = jnp.exp(jax.random.uniform(jax.random.fold_in(own, axis_at), (parts,), jnp.float32, smallest / len(pieces), largest / len(pieces)))
        factor_of = factor_of * jnp.repeat(heights, shape[axis_at] // parts).reshape([-1 if axis == axis_at else 1 for axis in range(len(shape))])
    return factor_of


def gaussian(stream_key, extent, scale, reach, split=(), kind=jnp.bfloat16):
    result = jax.random.normal(stream_key, extent, jnp.float32) * scale
    if len(split) > 0:
        result = levels(stream_key, extent, split, -0.22, 0.18) * result
    return jnp.clip(result, min=-reach, max=reach).astype(kind)


def setup_inputs(seed: int = 0) -> dict:
    splits = jax.random.split(jax.random.key(seed), 11)
    return {
        "coeffs": gaussian(splits[0], (S, C * P_SIZE), 1.0, 6.0, ((0, 256),)),
        "neighbours": place_ends(jax.random.randint(splits[1], (S, K), 0, 3 * SD), jax.random.fold_in(splits[1], 1), 0, (3 * SD) - 1).astype(jnp.int32),
        "counts": place_ends(jax.random.randint(splits[2], (S,), K // 4, K + 1), jax.random.fold_in(splits[2], 1), K // 4, K).astype(jnp.int32),
        "boxes": place_ends(jax.random.randint(splits[3], (S,), 0, NBC), jax.random.fold_in(splits[3], 1), 0, NBC - 1).astype(jnp.int32),
        "axial": gaussian(splits[4], (S, K, C), 0.18, 1.0, ((0, 256),)),
        "rotations": gaussian(splits[5], (K, C, C), C ** -0.5, 0.625),
        "out_map": gaussian(splits[6], (C, C), C ** -0.5, 0.625),
        "coupling": draw_coupling(jax.random.fold_in(splits[10], 71), 0),
        "in_map": gaussian(splits[8], (C, C), (C * BOX_SPH) ** -0.5, 0.21875),
        "tmat": jnp.clip(jax.random.uniform(splits[9], (S, C), jnp.float32, -0.5, 0.5) * levels(splits[9], (S, C), ((0, 256),), -0.4, 0.0), -0.5, 0.5),
    }


slot_width = 8


def near_field(cand, nbr, cnt, axial, rot):
    sd, slots = nbr.shape
    width = rot.shape[1]
    incid = cand.shape[1] // width
    groups = slots // slot_width
    live = (lax.broadcasted_iota(jnp.int32, (sd, slots), 1) < cnt[:, None]).astype(jnp.float32)
    scale = axial.astype(jnp.float32) * live[:, :, None]
    idx_groups = nbr.reshape(sd, groups, slot_width).transpose(1, 0, 2)
    scale_groups = scale.reshape(sd, groups, slot_width, width).transpose(1, 0, 2, 3)
    rot_groups = rot.reshape(groups, slot_width, width, width)

    def step(total, item):
        idx, factor, rg = item
        picked = cand[idx].reshape(sd, slot_width, width, incid)
        rg32 = rg.astype(jnp.float32)
        turned = jnp.einsum('kdc,skcp->skdp', rg32, picked.astype(jnp.float32))
        scaled = (turned * factor[..., None]).astype(jnp.bfloat16)
        back = jnp.einsum('kdc,skdp->scp', rg32, scaled.astype(jnp.float32))
        return total + back, None

    start = jnp.zeros((sd, width, incid), jnp.float32)
    total, _ = lax.scan(step, start, (idx_groups, scale_groups, rot_groups))
    return total


def apply_tmat(field, tmat):
    half = field.shape[1] // 2
    real_t = tmat[:, :half, None]
    imag_t = tmat[:, half:, None]
    real_u = field[:, :half]
    imag_u = field[:, half:]
    return jnp.concatenate([real_t * real_u - imag_t * imag_u, real_t * imag_u + imag_t * real_u], axis=1)


def reference(coeffs, neighbours, counts, boxes, axial, rotations, out_map, coupling, in_map, tmat):
    ncell = N_CELLS
    ngrp = N_GRP
    total = coeffs.shape[0]
    blocks = ncell * ngrp
    sd = total // blocks
    width = rotations.shape[1]
    incid = coeffs.shape[1] // width
    nbc = NBG * ngrp
    x4 = coeffs.reshape(ncell, ngrp, sd, width * incid)
    zero = jnp.zeros((1, ngrp, sd, width * incid), jnp.bfloat16)
    before = jnp.concatenate([zero, x4[:-1]], axis=0)
    after = jnp.concatenate([x4[1:], zero], axis=0)
    cand = jnp.concatenate([before, x4, after], axis=2).reshape(blocks, 3 * sd, width * incid)

    def one_block(item):
        cb, nb, cn, ax = item
        return near_field(cb, nb, cn, ax, rotations)

    near = lax.map(one_block, (cand, neighbours.reshape(blocks, sd, -1), counts.reshape(blocks, sd),
                               axial.reshape(blocks, sd, -1, width)))
    near = near.reshape(total, width, incid)

    onehot = (boxes.reshape(ncell, ngrp * sd)[:, :, None] == jnp.arange(nbc, dtype=jnp.int32)[None, None, :]).astype(jnp.float32)
    xcol = coeffs.reshape(ncell, ngrp * sd, width * incid).astype(jnp.float32)
    sums = jnp.einsum('nsb,nsq->nbq', onehot, xcol, precision=lax.Precision.HIGHEST)
    sums = sums.reshape(ncell, nbc, width, incid)
    moments = jnp.einsum('dc,nbcp->nbdp', out_map.astype(jnp.float32), sums, precision=lax.Precision.HIGHEST).astype(jnp.bfloat16)
    moments = moments.reshape(ncell * nbc, width * incid)
    local = jnp.dot(coupling, moments, preferred_element_type=jnp.float32).astype(jnp.bfloat16)
    local = local.reshape(ncell, nbc, width * incid).astype(jnp.float32)
    chosen = jnp.einsum('nsb,nbq->nsq', onehot, local, precision=lax.Precision.HIGHEST)
    chosen = chosen.reshape(total, width, incid)
    far = jnp.einsum('dc,scp->sdp', in_map.astype(jnp.float32), chosen, precision=lax.Precision.HIGHEST)
    field = near + far
    turned = apply_tmat(field, tmat).reshape(total, width * incid)
    return (coeffs.astype(jnp.float32) - turned).astype(jnp.bfloat16)
```

```python
import jax
import jax.numpy as jnp
from jax import lax
from jax.experimental import pallas as pl
from jax.experimental.pallas import tpu as pltpu
from jax.sharding import PartitionSpec as P

F32 = jnp.float32
BF16 = jnp.bfloat16
NBG = 2
LANES = 128
HALF = 64


def dot(a, b, ca=1, cb=0):
    return lax.dot_general(a, b, (((ca,), (cb,)), ((), ())), preferred_element_type=F32)


def params():
    return pltpu.CompilerParams(vmem_limit_bytes=48 * 1024 * 1024)


def to_planes(rows, planes, base):
    sd, width = rows.shape
    for t in range(width // LANES):
        planes[pl.ds(base * HALF + t, sd, stride=HALF), :] = rows[:, t * LANES:(t + 1) * LANES].astype(F32)


def pack_kernel(x, boxes, out):
    ngrp = out.shape[0]
    feat = x.shape[1] // ngrp
    tag = boxes[...]
    for g in range(ngrp):
        out[g, :, :feat] = x[:, g * feat:(g + 1) * feat]
        out[g, :, feat:] = tag


def pack(coeffs, boxes, ngrp):
    sd, width = coeffs.shape
    tag = jnp.broadcast_to(boxes.astype(BF16)[:, None], (sd, LANES))
    return pl.pallas_call(
        pack_kernel,
        out_shape=jax.ShapeDtypeStruct((ngrp, sd, width // ngrp + LANES), BF16),
        compiler_params=params(),
        name="pack",
    )(coeffs, tag)


def sums_kernel(got, out, onehot, *, nbc):
    n, sd, wide = got.shape
    feat = wide - LANES
    flat = got[...].reshape(n * sd, wide)
    box = flat[:, feat:feat + nbc].astype(F32)
    ids = lax.broadcasted_iota(jnp.int32, (n * sd, nbc), 1).astype(F32)
    hot = (box == ids).astype(F32).astype(BF16)
    onehot[...] = hot
    sums = dot(hot, flat[:, :feat], 0, 0).astype(BF16)
    for c in range(out.shape[0]):
        out[c] = sums


def box_sums(got, nbc, ncell):
    n, sd, wide = got.shape
    import functools
    return pl.pallas_call(
        functools.partial(sums_kernel, nbc=nbc),
        out_shape=(
            jax.ShapeDtypeStruct((ncell, nbc, wide - LANES), BF16),
            jax.ShapeDtypeStruct((n * sd, nbc), BF16),
        ),
        compiler_params=params(),
        name="box_sums",
    )(got)


def rows_kernel(column, onehot, coupling, out):
    out[...] = dot(onehot[...], coupling[...]).astype(BF16)


def sphere_rows(column, onehot, coupling):
    n, nbc = onehot.shape
    nbox = coupling.shape[1]
    return pl.pallas_call(
        rows_kernel,
        out_shape=jax.ShapeDtypeStruct((n, nbox), BF16),
        grid_spec=pltpu.PrefetchScalarGridSpec(
            num_scalar_prefetch=1,
            grid=(1,),
            in_specs=[
                pl.BlockSpec((n, nbc), lambda i, c: (0, 0)),
                pl.BlockSpec((nbc, nbox), lambda i, c: (c[0], 0)),
            ],
            out_specs=pl.BlockSpec((n, nbox), lambda i, c: (0, 0)),
        ),
        compiler_params=params(),
        name="sphere_rows",
    )(column, onehot, coupling)


def couple_kernel(rows, sums, out):
    nbox = rows.shape[1]
    feat = sums.shape[2]
    n, sd = out.shape[0], out.shape[1]
    out[...] = dot(rows[...], sums[...].reshape(nbox, feat)).astype(BF16).reshape(n, sd, feat)


def couple(rows, sums, n, sd):
    return pl.pallas_call(
        couple_kernel,
        out_shape=jax.ShapeDtypeStruct((n, sd, sums.shape[2]), BF16),
        compiler_params=params(),
        name="couple",
    )(rows, sums)


def swap_halves(a):
    return pltpu.roll(a, HALF, 1)


def near_kernel(nbr, low, own, high, scale, rot, perm, out, planes, cand, turn, diag, total):
    slots, sd, _ = scale.shape
    width = rot.shape[1]
    tiles = low.shape[1] // LANES
    lane = lax.broadcasted_iota(jnp.int32, (HALF, LANES), 1) < HALF
    turn[...] = jnp.zeros_like(turn)
    diag[...] = jnp.zeros_like(diag)
    for k in range(slots):
        turn[k * LANES:k * LANES + width, :] = dot(rot[k], perm[...]).astype(BF16)
    planes[...] = jnp.zeros_like(planes)
    for c, part in enumerate((low, own, high)):
        to_planes(part, planes, 0)
        for s in range(0, sd, 2):
            both = planes[s * HALF:(s + 2) * HALF, :].T
            top, bottom = both[:HALF], both[HALF:]
            cand[c * sd + s] = jnp.where(lane, top, swap_halves(bottom)).astype(BF16)
            cand[c * sd + s + 1] = jnp.where(lane, swap_halves(top), bottom).astype(BF16)
    total[...] = jnp.zeros_like(total)
    group = 4

    def step(q, carry):
        k = 2 * q
        r = pl.multiple_of(q * 2 * LANES, 2 * LANES)
        diag[:LANES, :LANES] = turn[pl.ds(r, LANES), :]
        diag[LANES:, LANES:] = turn[pl.ds(r + LANES, LANES), :]
        fact0 = scale[k]
        fact1 = scale[k + 1]
        back = turn[pl.ds(r, 2 * LANES), :]
        fwd = diag[...]
        for g in range(sd // group):
            picked = []
            for s in range(g * group, (g + 1) * group):
                a = cand[nbr[s, k]]
                b = cand[nbr[s, k + 1]]
                picked.append(jnp.concatenate([a, b], axis=1))
            turned = dot(jnp.concatenate(picked, axis=0), fwd, 1, 1)
            scaled = []
            for n, s in enumerate(range(g * group, (g + 1) * group)):
                f = jnp.concatenate([fact0[s:s + 1], fact1[s:s + 1]], axis=1)
                scaled.append((turned[n * HALF:(n + 1) * HALF] * f).astype(BF16))
            rows = pl.ds(g * group * HALF, group * HALF)
            total[rows, :] += dot(jnp.concatenate(scaled, axis=0), back)
        return carry

    lax.fori_loop(0, slots // 2, step, 0)
    for s in range(0, sd, 2):
        a = total[s * HALF:(s + 1) * HALF, :]
        b = total[(s + 1) * HALF:(s + 2) * HALF, :]
        top = jnp.where(lane, a, swap_halves(b))
        bottom = jnp.where(lane, swap_halves(a), b)
        out[s * HALF:(s + 2) * HALF, :] = jnp.concatenate([top, bottom], axis=0).T


def near_field(nbr, low, own, high, scale, rot, perm):
    slots, sd, _ = scale.shape
    vmem = pl.BlockSpec(memory_space=pltpu.VMEM)
    return pl.pallas_call(
        near_kernel,
        out_shape=jax.ShapeDtypeStruct((sd * HALF, LANES), F32),
        in_specs=[pl.BlockSpec(memory_space=pltpu.SMEM)] + [vmem] * 6,
        out_specs=vmem,
        scratch_shapes=[
            pltpu.VMEM((sd * HALF, LANES), F32),
            pltpu.VMEM((3 * sd, HALF, LANES), BF16),
            pltpu.VMEM((slots * LANES, LANES), BF16),
            pltpu.VMEM((2 * LANES, 2 * LANES), BF16),
            pltpu.VMEM((sd * HALF, LANES), F32),
        ],
        compiler_params=params(),
        name="near",
    )(nbr, low, own, high, scale, rot, perm)


def tail_kernel(got, near, x, tmat_re, tmat_im, maps, out, planes):
    ngrp, sd, feat = got.shape
    per = feat // LANES
    lane = lax.broadcasted_iota(jnp.int32, (HALF, LANES), 1) < HALF
    half = tmat_re.shape[1]
    planes[...] = jnp.zeros_like(planes)
    for g in range(ngrp):
        part = got[g]
        for q in range(per):
            t = g * per + q
            planes[pl.ds(t, sd, stride=HALF), :] = part[:, q * LANES:(q + 1) * LANES].astype(F32)
    hi = maps[:LANES]
    lo = maps[LANES:]
    for s in range(sd):
        loc = planes[s * HALF:(s + 1) * HALF, :]
        both = jnp.concatenate([loc, swap_halves(loc)], axis=0).astype(BF16)
        prod = dot(hi, both) + dot(lo, both)
        field = near[s * HALF:(s + 1) * HALF, :] + jnp.where(lane, prod[:HALF], prod[HALF:])
        ur, ui = field[:half], field[half:2 * half]
        tr, ti = tmat_re[s], tmat_im[s]
        planes[s * HALF:s * HALF + half, :] = tr * ur - ti * ui
        planes[s * HALF + half:s * HALF + 2 * half, :] = tr * ui + ti * ur
    for t in range(2 * half):
        cols = slice(t * LANES, (t + 1) * LANES)
        out[:, cols] = (x[:, cols].astype(F32) - planes[pl.ds(t, sd, stride=HALF), :]).astype(BF16)


def tail(got, near, coeffs, tmat_re, tmat_im, maps):
    sd = coeffs.shape[0]
    return pl.pallas_call(
        tail_kernel,
        out_shape=jax.ShapeDtypeStruct(coeffs.shape, BF16),
        scratch_shapes=[pltpu.VMEM((sd * HALF, LANES), F32)],
        compiler_params=params(),
        name="tail",
    )(got, near, coeffs, tmat_re, tmat_im, maps)


def plane_maps(out_map, in_map):
    both = jnp.dot(in_map.astype(F32), out_map.astype(F32), precision=lax.Precision.HIGHEST)
    n = both.shape[0] // 2
    m = both.reshape(n, 2, n, 2)
    pad = ((0, HALF - n), (0, HALF - n))
    ee, eo, oe, oo = (jnp.pad(m[:, i, :, j], pad) for i in (0, 1) for j in (0, 1))
    top = jnp.concatenate([ee, eo], axis=1)
    bottom = jnp.concatenate([oo, oe], axis=1)
    full = jnp.concatenate([top, bottom], axis=0)
    hi = lax.reduce_precision(full, 8, 7)
    return jnp.concatenate([hi, full - hi], axis=0).astype(BF16)


def shards(coeffs, neighbours, counts, boxes, axial, rotations, out_map, coupling, in_map, tmat):
    sd, total = coeffs.shape
    width = rotations.shape[1]
    slots = neighbours.shape[1]
    ngrp = lax.axis_size("grp")
    ncell = lax.axis_size("cells")
    nbc = NBG * ngrp
    forward = [(i, i + 1) for i in range(ncell - 1)]
    backward = [(b, a) for a, b in forward]
    low = lax.ppermute(coeffs, "cells", forward)
    high = lax.ppermute(coeffs, "cells", backward)

    sent = pack(coeffs, boxes, ngrp)
    got = lax.all_to_all(sent, "grp", 0, 0, tiled=True)
    sums, onehot = box_sums(got, nbc, ncell)
    every = lax.all_to_all(sums, "cells", 0, 0, tiled=True)
    column = lax.axis_index("cells").astype(jnp.int32)[None]
    rows = sphere_rows(column, onehot, coupling)

    live = lax.broadcasted_iota(jnp.int32, (sd, slots), 1) < counts[:, None]
    scale = jnp.where(live[:, :, None], axial.astype(F32), 0.0).transpose(1, 0, 2)
    scale = jnp.pad(scale, ((0, 0), (0, 0), (0, LANES - width)))
    spot = jnp.arange(width, dtype=jnp.int32)
    spot = (spot % 2) * HALF + spot // 2
    perm = (spot[:, None] == jnp.arange(LANES, dtype=jnp.int32)[None, :]).astype(BF16)
    near = near_field(neighbours, low, coeffs, high, scale, rotations, perm)

    local = couple(rows, every, ngrp, sd)
    mine = lax.all_to_all(local, "grp", 0, 0, tiled=True)
    spread = jnp.repeat(tmat.reshape(sd, width // 2, 2), HALF, axis=2)
    quarter = width // 4
    return tail(mine, near, coeffs, spread[:, :quarter], spread[:, quarter:], plane_maps(out_map, in_map))


def solution(mesh):
    rows = P(("cells", "grp"), None)
    flat = P(("cells", "grp"))
    in_specs = (rows, rows, flat, flat, P(("cells", "grp"), None, None), P(), P(), P(), P(), rows)
    return jax.shard_map(shards, mesh=mesh, in_specs=in_specs, out_specs=rows, check_vma=False)
```

```python
import functools

import jax
import jax.numpy as jnp
from jax import lax
from jax.experimental import pallas as pl
from jax.experimental.pallas import tpu as pltpu
from jax.sharding import PartitionSpec as P


F32 = jnp.float32
BF16 = jnp.bfloat16
NBG = 2
LANES = 128
HALF = 64


def dot(a, b, ca=1, cb=0):
    return lax.dot_general(a, b, (((ca,), (cb,)), ((), ())), preferred_element_type=F32)


def params():
    return pltpu.CompilerParams(vmem_limit_bytes=12 * 1024 * 1024)


def to_planes(rows, planes, base):
    sd, width = rows.shape
    for t in range(width // LANES):
        planes[pl.ds(base * HALF + t, sd, stride=HALF), :] = rows[:, t * LANES:(t + 1) * LANES].astype(F32)


def swap_halves(a):
    return pltpu.roll(a, HALF, 1)


def pack_kernel(x, boxes, out):
    ngrp = out.shape[0]
    feat = x.shape[1] // ngrp
    tag = boxes[...]
    for g in range(ngrp):
        out[g, :, :feat] = x[:, g * feat:(g + 1) * feat]
        out[g, :, feat:] = tag


def pack(coeffs, boxes, ngrp):
    sd, width = coeffs.shape
    tag = jnp.broadcast_to(boxes.astype(BF16)[:, None], (sd, LANES))
    return pl.pallas_call(
        pack_kernel,
        out_shape=jax.ShapeDtypeStruct((ngrp, sd, width // ngrp + LANES), BF16),
        compiler_params=params(),
        name="pack",
    )(coeffs, tag)


def sums_kernel(got, out, onehot, *, nbc):
    n, sd, wide = got.shape
    feat = wide - LANES
    flat = got[...].reshape(n * sd, wide)
    box = flat[:, feat:feat + nbc].astype(F32)
    ids = lax.broadcasted_iota(jnp.int32, (n * sd, nbc), 1).astype(F32)
    hot = (box == ids).astype(F32).astype(BF16)
    onehot[...] = hot
    sums = dot(hot, flat[:, :feat], 0, 0).astype(BF16)
    for c in range(out.shape[0]):
        out[c] = sums


def box_sums(got, nbc, ncell):
    n, sd, wide = got.shape
    return pl.pallas_call(
        functools.partial(sums_kernel, nbc=nbc),
        out_shape=(
            jax.ShapeDtypeStruct((ncell, nbc, wide - LANES), BF16),
            jax.ShapeDtypeStruct((n * sd, nbc), BF16),
        ),
        compiler_params=params(),
        name="box_sums",
    )(got)


def rows_kernel(column, onehot, coupling, out):
    out[...] = dot(onehot[...], coupling[...]).astype(BF16)


def sphere_rows(column, onehot, coupling):
    n, nbc = onehot.shape
    nbox = coupling.shape[1]
    return pl.pallas_call(
        rows_kernel,
        out_shape=jax.ShapeDtypeStruct((n, nbox), BF16),
        grid_spec=pltpu.PrefetchScalarGridSpec(
            num_scalar_prefetch=1,
            grid=(1,),
            in_specs=[
                pl.BlockSpec((n, nbc), lambda i, c: (0, 0)),
                pl.BlockSpec((nbc, nbox), lambda i, c: (c[0], 0)),
            ],
            out_specs=pl.BlockSpec((n, nbox), lambda i, c: (0, 0)),
        ),
        compiler_params=params(),
        name="sphere_rows",
    )(column, onehot, coupling)


def couple_kernel(rows, sums, out):
    nbox = rows.shape[1]
    feat = sums.shape[2]
    n, sd = out.shape[0], out.shape[1]
    out[...] = dot(rows[...], sums[...].reshape(nbox, feat)).astype(BF16).reshape(n, sd, feat)


def couple(rows, sums, n, sd):
    return pl.pallas_call(
        couple_kernel,
        out_shape=jax.ShapeDtypeStruct((n, sd, sums.shape[2]), BF16),
        compiler_params=params(),
        name="couple",
    )(rows, sums)


def prep_kernel(counts, axial, rot, perm, permt, out_map, in_map, tmat, turn, scale, maps, tre, tim, cols):
    sd, slots, width = axial.shape
    n = width // 2
    turn[...] = jnp.zeros_like(turn)
    for k in range(slots):
        turn[k * LANES:k * LANES + width, :] = dot(rot[k], perm[...]).astype(BF16)
    slot = lax.broadcasted_iota(jnp.int32, (slots, LANES), 0)
    pad = jnp.zeros((slots, LANES - width), F32)
    for i in range(sd):
        factor = jnp.concatenate([axial[i].astype(F32), pad], axis=1)
        scale[pl.ds(i, slots, stride=sd), :] = jnp.where(slot < counts[i], factor, 0.0)
    both = dot(in_map[...], out_map[...])
    hi = both.astype(BF16)
    lo = (both - hi.astype(F32)).astype(BF16)
    for r, part in enumerate((hi, lo)):
        moved = dot(dot(permt[...], part).astype(BF16), perm[...])
        maps[r * LANES:r * LANES + HALF, :] = moved[:HALF].astype(BF16)
        maps[r * LANES + HALF:(r + 1) * LANES, :] = swap_halves(moved[HALF:]).astype(BF16)
    cols[...] = tmat[...].T
    lane = lax.broadcasted_iota(jnp.int32, (n, LANES), 1) < HALF
    even = cols[pl.ds(0, n, stride=2), :]
    odd = cols[pl.ds(1, n, stride=2), :]
    for i in range(sd):
        row = jnp.where(lane, even[:, i:i + 1], odd[:, i:i + 1])
        tre[i] = row[:n // 2]
        tim[i] = row[n // 2:]


def prepare(counts, axial, rot, perm, permt, out_map, in_map, tmat):
    sd, slots, width = axial.shape
    vmem = pl.BlockSpec(memory_space=pltpu.VMEM)
    spread = jax.ShapeDtypeStruct((sd, width // 4, LANES), F32)
    return pl.pallas_call(
        prep_kernel,
        out_shape=(
            jax.ShapeDtypeStruct((slots * LANES, LANES), BF16),
            jax.ShapeDtypeStruct((slots * sd, LANES), F32),
            jax.ShapeDtypeStruct((2 * LANES, LANES), BF16),
            spread,
            spread,
        ),
        in_specs=[pl.BlockSpec(memory_space=pltpu.SMEM)] + [vmem] * 7,
        scratch_shapes=[pltpu.VMEM((width, sd), F32)],
        compiler_params=params(),
        name="prepare",
    )(counts, axial, rot, perm, permt, out_map, in_map, tmat)


def near_kernel(nbr, low, own, high, scale, turn, out, planes, cand, diag, total):
    sd, slots = nbr.shape
    lane = lax.broadcasted_iota(jnp.int32, (HALF, LANES), 1) < HALF
    diag[...] = jnp.zeros_like(diag)
    planes[...] = jnp.zeros_like(planes)
    for c, part in enumerate((low, own, high)):
        to_planes(part, planes, 0)
        for s in range(0, sd, 2):
            both = planes[s * HALF:(s + 2) * HALF, :].T
            top, bottom = both[:HALF], both[HALF:]
            cand[c * sd + s] = jnp.where(lane, top, swap_halves(bottom)).astype(BF16)
            cand[c * sd + s + 1] = jnp.where(lane, swap_halves(top), bottom).astype(BF16)
    total[...] = jnp.zeros_like(total)
    group = 4

    def step(q, carry):
        k = 2 * q
        r = pl.multiple_of(q * 2 * LANES, 2 * LANES)
        diag[:LANES, :LANES] = turn[pl.ds(r, LANES), :]
        diag[LANES:, LANES:] = turn[pl.ds(r + LANES, LANES), :]
        fact0 = scale[pl.ds(pl.multiple_of(k * sd, sd), sd), :]
        fact1 = scale[pl.ds(pl.multiple_of(k * sd + sd, sd), sd), :]
        back = turn[pl.ds(r, 2 * LANES), :]
        fwd = diag[...]
        for g in range(sd // group):
            picked = []
            for s in range(g * group, (g + 1) * group):
                a = cand[nbr[s, k]]
                b = cand[nbr[s, k + 1]]
                picked.append(jnp.concatenate([a, b], axis=1))
            turned = dot(jnp.concatenate(picked, axis=0), fwd, 1, 1)
            scaled = []
            for n, s in enumerate(range(g * group, (g + 1) * group)):
                f = jnp.concatenate([fact0[s:s + 1], fact1[s:s + 1]], axis=1)
                scaled.append((turned[n * HALF:(n + 1) * HALF] * f).astype(BF16))
            rows = pl.ds(g * group * HALF, group * HALF)
            total[rows, :] += dot(jnp.concatenate(scaled, axis=0), back)
        return carry

    lax.fori_loop(0, slots // 2, step, 0)
    for s in range(0, sd, 2):
        a = total[s * HALF:(s + 1) * HALF, :]
        b = total[(s + 1) * HALF:(s + 2) * HALF, :]
        top = jnp.where(lane, a, swap_halves(b))
        bottom = jnp.where(lane, swap_halves(a), b)
        out[s * HALF:(s + 2) * HALF, :] = jnp.concatenate([top, bottom], axis=0).T


def near_field(nbr, low, own, high, scale, turn):
    sd, _ = nbr.shape
    vmem = pl.BlockSpec(memory_space=pltpu.VMEM)
    return pl.pallas_call(
        near_kernel,
        out_shape=jax.ShapeDtypeStruct((sd * HALF, LANES), F32),
        in_specs=[pl.BlockSpec(memory_space=pltpu.SMEM)] + [vmem] * 5,
        out_specs=vmem,
        scratch_shapes=[
            pltpu.VMEM((sd * HALF, LANES), F32),
            pltpu.VMEM((3 * sd, HALF, LANES), BF16),
            pltpu.VMEM((2 * LANES, 2 * LANES), BF16),
            pltpu.VMEM((sd * HALF, LANES), F32),
        ],
        compiler_params=params(),
        name="near",
    )(nbr, low, own, high, scale, turn)


def tail_kernel(got, near, x, tmat_re, tmat_im, maps, out, planes):
    ngrp, sd, feat = got.shape
    per = feat // LANES
    lane = lax.broadcasted_iota(jnp.int32, (HALF, LANES), 1) < HALF
    half = tmat_re.shape[1]
    planes[...] = jnp.zeros_like(planes)
    for g in range(ngrp):
        part = got[g]
        for q in range(per):
            t = g * per + q
            planes[pl.ds(t, sd, stride=HALF), :] = part[:, q * LANES:(q + 1) * LANES].astype(F32)
    hi = maps[:LANES]
    lo = maps[LANES:]
    for s in range(sd):
        loc = planes[s * HALF:(s + 1) * HALF, :]
        both = jnp.concatenate([loc, swap_halves(loc)], axis=0).astype(BF16)
        prod = dot(hi, both) + dot(lo, both)
        field = near[s * HALF:(s + 1) * HALF, :] + jnp.where(lane, prod[:HALF], prod[HALF:])
        ur, ui = field[:half], field[half:2 * half]
        tr, ti = tmat_re[s], tmat_im[s]
        planes[s * HALF:s * HALF + half, :] = tr * ur - ti * ui
        planes[s * HALF + half:s * HALF + 2 * half, :] = tr * ui + ti * ur
    for t in range(2 * half):
        cols = slice(t * LANES, (t + 1) * LANES)
        out[:, cols] = (x[:, cols].astype(F32) - planes[pl.ds(t, sd, stride=HALF), :]).astype(BF16)


def tail(got, near, coeffs, tmat_re, tmat_im, maps):
    sd = coeffs.shape[0]
    return pl.pallas_call(
        tail_kernel,
        out_shape=jax.ShapeDtypeStruct(coeffs.shape, BF16),
        scratch_shapes=[pltpu.VMEM((sd * HALF, LANES), F32)],
        compiler_params=params(),
        name="tail",
    )(got, near, coeffs, tmat_re, tmat_im, maps)


def shards(coeffs, neighbours, counts, boxes, axial, rotations, out_map, coupling, in_map, tmat):
    sd, _ = coeffs.shape
    width = rotations.shape[1]
    ngrp = lax.axis_size("grp")
    ncell = lax.axis_size("cells")
    nbc = NBG * ngrp
    forward = [(i, i + 1) for i in range(ncell - 1)]
    backward = [(b, a) for a, b in forward]
    low = lax.ppermute(coeffs, "cells", forward)
    high = lax.ppermute(coeffs, "cells", backward)
    sent = pack(coeffs, boxes, ngrp)
    got = lax.all_to_all(sent, "grp", 0, 0, tiled=True)
    spot = jnp.arange(width, dtype=jnp.int32)
    spot = (spot % 2) * HALF + spot // 2
    lanes = jnp.arange(LANES, dtype=jnp.int32)
    perm = (spot[:, None] == lanes[None, :]).astype(BF16)
    permt = (lanes[:, None] == spot[None, :]).astype(BF16)
    turn, scale, maps, tre, tim = prepare(
        counts, axial, rotations, perm, permt, out_map, in_map, tmat
    )
    sums, onehot = box_sums(got, nbc, ncell)
    every = lax.all_to_all(sums, "cells", 0, 0, tiled=True)
    column = lax.axis_index("cells").astype(jnp.int32)[None]
    rows = sphere_rows(column, onehot, coupling)
    near = near_field(neighbours, low, coeffs, high, scale, turn)
    local = couple(rows, every, ngrp, sd)
    mine = lax.all_to_all(local, "grp", 0, 0, tiled=True)
    return tail(mine, near, coeffs, tre, tim, maps)


def solution(mesh):
    rows = P(("cells", "grp"), None)
    flat = P(("cells", "grp"))
    in_specs = (rows, rows, flat, flat, P(("cells", "grp"), None, None), P(), P(), P(), P(), rows)
    return jax.shard_map(shards, mesh=mesh, in_specs=in_specs, out_specs=rows, check_vma=False)
```

```python
import functools

import jax
import jax.numpy as jnp
from jax import lax
from jax.experimental import pallas as pl
from jax.experimental.pallas import tpu as pltpu
from jax.sharding import PartitionSpec as P


F32 = jnp.float32
BF16 = jnp.bfloat16
NBG = 2
LANES = 128
HALF = 64
UNROLL = 4


def dot(a, b, ca=1, cb=0):
    return lax.dot_general(a, b, (((ca,), (cb,)), ((), ())), preferred_element_type=F32)


def params():
    return pltpu.CompilerParams(vmem_limit_bytes=12 * 1024 * 1024)


def to_planes(rows, planes, base):
    sd, width = rows.shape
    for t in range(width // LANES):
        planes[pl.ds(base * HALF + t, sd, stride=HALF), :] = rows[:, t * LANES:(t + 1) * LANES].astype(F32)


def swap_halves(a):
    return pltpu.roll(a, HALF, 1)


def pack_kernel(x, boxes, out):
    ngrp = out.shape[0]
    feat = x.shape[1] // ngrp
    tag = boxes[...]
    for g in range(ngrp):
        out[g, :, :feat] = x[:, g * feat:(g + 1) * feat]
        out[g, :, feat:] = tag


def pack(coeffs, boxes, ngrp):
    sd, width = coeffs.shape
    tag = jnp.broadcast_to(boxes.astype(BF16)[:, None], (sd, LANES))
    return pl.pallas_call(
        pack_kernel,
        out_shape=jax.ShapeDtypeStruct((ngrp, sd, width // ngrp + LANES), BF16),
        compiler_params=params(),
        name="pack",
    )(coeffs, tag)


def sums_kernel(got, out, onehot, *, nbc):
    n, sd, wide = got.shape
    feat = wide - LANES
    flat = got[...].reshape(n * sd, wide)
    box = flat[:, feat:feat + nbc].astype(F32)
    ids = lax.broadcasted_iota(jnp.int32, (n * sd, nbc), 1).astype(F32)
    hot = (box == ids).astype(F32).astype(BF16)
    onehot[...] = hot
    sums = dot(hot, flat[:, :feat], 0, 0).astype(BF16)
    for c in range(out.shape[0]):
        out[c] = sums


def box_sums(got, nbc, ncell):
    n, sd, wide = got.shape
    return pl.pallas_call(
        functools.partial(sums_kernel, nbc=nbc),
        out_shape=(
            jax.ShapeDtypeStruct((ncell, nbc, wide - LANES), BF16),
            jax.ShapeDtypeStruct((n * sd, nbc), BF16),
        ),
        compiler_params=params(),
        name="box_sums",
    )(got)


def rows_kernel(column, onehot, coupling, out):
    out[...] = dot(onehot[...], coupling[...]).astype(BF16)


def sphere_rows(column, onehot, coupling):
    n, nbc = onehot.shape
    nbox = coupling.shape[1]
    return pl.pallas_call(
        rows_kernel,
        out_shape=jax.ShapeDtypeStruct((n, nbox), BF16),
        grid_spec=pltpu.PrefetchScalarGridSpec(
            num_scalar_prefetch=1,
            grid=(1,),
            in_specs=[
                pl.BlockSpec((n, nbc), lambda i, c: (0, 0)),
                pl.BlockSpec((nbc, nbox), lambda i, c: (c[0], 0)),
            ],
            out_specs=pl.BlockSpec((n, nbox), lambda i, c: (0, 0)),
        ),
        compiler_params=params(),
        name="sphere_rows",
    )(column, onehot, coupling)


def couple_kernel(rows, sums, out):
    nbox = rows.shape[1]
    feat = sums.shape[2]
    n, sd = out.shape[0], out.shape[1]
    out[...] = dot(rows[...], sums[...].reshape(nbox, feat)).astype(BF16).reshape(n, sd, feat)


def couple(rows, sums, n, sd):
    return pl.pallas_call(
        couple_kernel,
        out_shape=jax.ShapeDtypeStruct((n, sd, sums.shape[2]), BF16),
        compiler_params=params(),
        name="couple",
    )(rows, sums)


def prep_kernel(counts, axial, rot, perm, permt, out_map, in_map, tmat, turn, scale, maps, tre, tim, cols):
    sd, slots, width = axial.shape
    n = width // 2
    turn[...] = jnp.zeros_like(turn)
    for k in range(slots):
        turn[k * LANES:k * LANES + width, :] = dot(rot[k], perm[...]).astype(BF16)
    slot = lax.broadcasted_iota(jnp.int32, (slots, LANES), 0)
    pad = jnp.zeros((slots, LANES - width), F32)
    for i in range(sd):
        factor = jnp.concatenate([axial[i].astype(F32), pad], axis=1)
        scale[pl.ds(i, slots, stride=sd), :] = jnp.where(slot < counts[i], factor, 0.0)
    both = dot(in_map[...], out_map[...])
    hi = both.astype(BF16)
    lo = (both - hi.astype(F32)).astype(BF16)
    for r, part in enumerate((hi, lo)):
        moved = dot(dot(permt[...], part).astype(BF16), perm[...])
        maps[r * LANES:r * LANES + HALF, :] = moved[:HALF].astype(BF16)
        maps[r * LANES + HALF:(r + 1) * LANES, :] = swap_halves(moved[HALF:]).astype(BF16)
    cols[...] = tmat[...].T
    lane = lax.broadcasted_iota(jnp.int32, (n, LANES), 1) < HALF
    even = cols[pl.ds(0, n, stride=2), :]
    odd = cols[pl.ds(1, n, stride=2), :]
    for i in range(sd):
        row = jnp.where(lane, even[:, i:i + 1], odd[:, i:i + 1])
        tre[i] = row[:n // 2]
        tim[i] = row[n // 2:]


def prepare(counts, axial, rot, perm, permt, out_map, in_map, tmat):
    sd, slots, width = axial.shape
    vmem = pl.BlockSpec(memory_space=pltpu.VMEM)
    spread = jax.ShapeDtypeStruct((sd, width // 4, LANES), F32)
    return pl.pallas_call(
        prep_kernel,
        out_shape=(
            jax.ShapeDtypeStruct((slots * LANES, LANES), BF16),
            jax.ShapeDtypeStruct((slots * sd, LANES), F32),
            jax.ShapeDtypeStruct((2 * LANES, LANES), BF16),
            spread,
            spread,
        ),
        in_specs=[pl.BlockSpec(memory_space=pltpu.SMEM)] + [vmem] * 7,
        scratch_shapes=[pltpu.VMEM((width, sd), F32)],
        compiler_params=params(),
        name="prepare",
    )(counts, axial, rot, perm, permt, out_map, in_map, tmat)


def near_kernel(nbr, low, own, high, scale, turn, out, sides, planes, cand, diag, total, sems):
    sd, slots = nbr.shape
    copies = [pltpu.make_async_copy(src, sides.at[n], sems.at[n]) for n, src in enumerate((low, high))]
    for copy in copies:
        copy.start()
    lane = lax.broadcasted_iota(jnp.int32, (HALF, LANES), 1) < HALF
    diag[...] = jnp.zeros_like(diag)
    planes[...] = jnp.zeros_like(planes)
    for c in (1, 0, 2):
        if c != 1:
            copies[c // 2].wait()
        to_planes(own if c == 1 else sides[c // 2], planes, 0)
        for s in range(0, sd, 2):
            both = planes[s * HALF:(s + 2) * HALF, :].T
            top, bottom = both[:HALF], both[HALF:]
            cand[c * sd + s] = jnp.where(lane, top, swap_halves(bottom)).astype(BF16)
            cand[c * sd + s + 1] = jnp.where(lane, swap_halves(top), bottom).astype(BF16)
    total[...] = jnp.zeros_like(total)
    group = 4

    def pair(q, diag):
        k = 2 * q
        r = pl.multiple_of(q * 2 * LANES, 2 * LANES)
        diag[:LANES, :LANES] = turn[pl.ds(r, LANES), :]
        diag[LANES:, LANES:] = turn[pl.ds(r + LANES, LANES), :]
        fact0 = scale[pl.ds(pl.multiple_of(k * sd, sd), sd), :]
        fact1 = scale[pl.ds(pl.multiple_of(k * sd + sd, sd), sd), :]
        back = turn[pl.ds(r, 2 * LANES), :]
        fwd = diag[...]
        for g in range(sd // group):
            picked = []
            for s in range(g * group, (g + 1) * group):
                a = cand[nbr[s, k]]
                b = cand[nbr[s, k + 1]]
                picked.append(jnp.concatenate([a, b], axis=1))
            turned = dot(jnp.concatenate(picked, axis=0), fwd, 1, 1)
            scaled = []
            for n, s in enumerate(range(g * group, (g + 1) * group)):
                f = jnp.concatenate([fact0[s:s + 1], fact1[s:s + 1]], axis=1)
                scaled.append((turned[n * HALF:(n + 1) * HALF] * f).astype(BF16))
            rows = pl.ds(g * group * HALF, group * HALF)
            total[rows, :] += dot(jnp.concatenate(scaled, axis=0), back)

    def step(m, carry):
        for u in range(UNROLL):
            pair(UNROLL * m + u, diag.at[u])
        return carry

    lax.fori_loop(0, slots // (2 * UNROLL), step, 0)
    for s in range(0, sd, 2):
        a = total[s * HALF:(s + 1) * HALF, :]
        b = total[(s + 1) * HALF:(s + 2) * HALF, :]
        top = jnp.where(lane, a, swap_halves(b))
        bottom = jnp.where(lane, swap_halves(a), b)
        out[s * HALF:(s + 2) * HALF, :] = jnp.concatenate([top, bottom], axis=0).T


def near_field(nbr, low, own, high, scale, turn):
    sd, _ = nbr.shape
    vmem = pl.BlockSpec(memory_space=pltpu.VMEM)
    place = pl.BlockSpec(memory_space=pl.ANY)
    return pl.pallas_call(
        near_kernel,
        out_shape=jax.ShapeDtypeStruct((sd * HALF, LANES), F32),
        in_specs=[pl.BlockSpec(memory_space=pltpu.SMEM), place, vmem, place, vmem, vmem],
        out_specs=vmem,
        scratch_shapes=[
            pltpu.VMEM((2, *own.shape), BF16),
            pltpu.VMEM((sd * HALF, LANES), F32),
            pltpu.VMEM((3 * sd, HALF, LANES), BF16),
            pltpu.VMEM((UNROLL, 2 * LANES, 2 * LANES), BF16),
            pltpu.VMEM((sd * HALF, LANES), F32),
            pltpu.SemaphoreType.DMA((2,)),
        ],
        compiler_params=params(),
        name="near",
    )(nbr, low, own, high, scale, turn)


def tail_kernel(got, near, x, tmat_re, tmat_im, maps, out, planes):
    ngrp, sd, feat = got.shape
    per = feat // LANES
    lane = lax.broadcasted_iota(jnp.int32, (HALF, LANES), 1) < HALF
    half = tmat_re.shape[1]
    planes[...] = jnp.zeros_like(planes)
    for g in range(ngrp):
        part = got[g]
        for q in range(per):
            t = g * per + q
            planes[pl.ds(t, sd, stride=HALF), :] = part[:, q * LANES:(q + 1) * LANES].astype(F32)
    hi = maps[:LANES]
    lo = maps[LANES:]
    for s in range(sd):
        loc = planes[s * HALF:(s + 1) * HALF, :]
        both = jnp.concatenate([loc, swap_halves(loc)], axis=0).astype(BF16)
        prod = dot(hi, both) + dot(lo, both)
        field = near[s * HALF:(s + 1) * HALF, :] + jnp.where(lane, prod[:HALF], prod[HALF:])
        ur, ui = field[:half], field[half:2 * half]
        tr, ti = tmat_re[s], tmat_im[s]
        planes[s * HALF:s * HALF + half, :] = tr * ur - ti * ui
        planes[s * HALF + half:s * HALF + 2 * half, :] = tr * ui + ti * ur
    for t in range(2 * half):
        cols = slice(t * LANES, (t + 1) * LANES)
        out[:, cols] = (x[:, cols].astype(F32) - planes[pl.ds(t, sd, stride=HALF), :]).astype(BF16)


def tail(got, near, coeffs, tmat_re, tmat_im, maps):
    sd = coeffs.shape[0]
    return pl.pallas_call(
        tail_kernel,
        out_shape=jax.ShapeDtypeStruct(coeffs.shape, BF16),
        scratch_shapes=[pltpu.VMEM((sd * HALF, LANES), F32)],
        compiler_params=params(),
        name="tail",
    )(got, near, coeffs, tmat_re, tmat_im, maps)


def shards(coeffs, neighbours, counts, boxes, axial, rotations, out_map, coupling, in_map, tmat):
    sd, _ = coeffs.shape
    width = rotations.shape[1]
    ngrp = lax.axis_size("grp")
    ncell = lax.axis_size("cells")
    nbc = NBG * ngrp
    forward = [(i, i + 1) for i in range(ncell - 1)]
    backward = [(b, a) for a, b in forward]
    low = lax.ppermute(coeffs, "cells", forward)
    high = lax.ppermute(coeffs, "cells", backward)
    sent = pack(coeffs, boxes, ngrp)
    got = lax.all_to_all(sent, "grp", 0, 0, tiled=True)
    spot = jnp.arange(width, dtype=jnp.int32)
    spot = (spot % 2) * HALF + spot // 2
    lanes = jnp.arange(LANES, dtype=jnp.int32)
    perm = (spot[:, None] == lanes[None, :]).astype(BF16)
    permt = (lanes[:, None] == spot[None, :]).astype(BF16)
    turn, scale, maps, tre, tim = prepare(
        counts, axial, rotations, perm, permt, out_map, in_map, tmat
    )
    sums, onehot = box_sums(got, nbc, ncell)
    every = lax.all_to_all(sums, "cells", 0, 0, tiled=True)
    column = lax.axis_index("cells").astype(jnp.int32)[None]
    rows = sphere_rows(column, onehot, coupling)
    near = near_field(neighbours, low, coeffs, high, scale, turn)
    local = couple(rows, every, ngrp, sd)
    mine = lax.all_to_all(local, "grp", 0, 0, tiled=True)
    return tail(mine, near, coeffs, tre, tim, maps)


def solution(mesh):
    rows = P(("cells", "grp"), None)
    flat = P(("cells", "grp"))
    in_specs = (rows, rows, flat, flat, P(("cells", "grp"), None, None), P(), P(), P(), P(), rows)
    return jax.shard_map(shards, mesh=mesh, in_specs=in_specs, out_specs=rows, check_vma=False)
```

```python
import functools

import jax
import jax.numpy as jnp
from jax import lax
from jax.experimental import pallas as pl
from jax.experimental.pallas import tpu as pltpu
from jax.sharding import PartitionSpec as P


F32 = jnp.float32
BF16 = jnp.bfloat16
NBG = 2
LANES = 128
HALF = 64
UNROLL = 4


def dot(a, b, ca=1, cb=0):
    return lax.dot_general(a, b, (((ca,), (cb,)), ((), ())), preferred_element_type=F32)


def params():
    return pltpu.CompilerParams(vmem_limit_bytes=12 * 1024 * 1024)


def to_planes(rows, planes, base):
    sd, width = rows.shape
    for t in range(width // LANES):
        planes[pl.ds(base * HALF + t, sd, stride=HALF), :] = rows[:, t * LANES:(t + 1) * LANES].astype(F32)


def swap_halves(a):
    return pltpu.roll(a, HALF, 1)


def pack_kernel(x, boxes, out):
    ngrp = out.shape[0]
    feat = x.shape[1] // ngrp
    tag = boxes[...]
    for g in range(ngrp):
        out[g, :, :feat] = x[:, g * feat:(g + 1) * feat]
        out[g, :, feat:] = tag


def pack(coeffs, boxes, ngrp):
    sd, width = coeffs.shape
    tag = jnp.broadcast_to(boxes.astype(BF16)[:, None], (sd, LANES))
    return pl.pallas_call(
        pack_kernel,
        out_shape=jax.ShapeDtypeStruct((ngrp, sd, width // ngrp + LANES), BF16),
        compiler_params=params(),
        name="pack",
    )(coeffs, tag)


def sums_kernel(got, out, onehot, *, nbc):
    n, sd, wide = got.shape
    feat = wide - LANES
    flat = got[...].reshape(n * sd, wide)
    box = flat[:, feat:feat + nbc].astype(F32)
    ids = lax.broadcasted_iota(jnp.int32, (n * sd, nbc), 1).astype(F32)
    hot = (box == ids).astype(F32).astype(BF16)
    onehot[...] = hot
    sums = dot(hot, flat[:, :feat], 0, 0).astype(BF16)
    for c in range(out.shape[0]):
        out[c] = sums


def box_sums(got, nbc, ncell):
    n, sd, wide = got.shape
    return pl.pallas_call(
        functools.partial(sums_kernel, nbc=nbc),
        out_shape=(
            jax.ShapeDtypeStruct((ncell, nbc, wide - LANES), BF16),
            jax.ShapeDtypeStruct((n * sd, nbc), BF16),
        ),
        compiler_params=params(),
        name="box_sums",
    )(got)


def rows_kernel(column, onehot, coupling, out):
    out[...] = dot(onehot[...], coupling[...]).astype(BF16)


def sphere_rows(column, onehot, coupling):
    n, nbc = onehot.shape
    nbox = coupling.shape[1]
    return pl.pallas_call(
        rows_kernel,
        out_shape=jax.ShapeDtypeStruct((n, nbox), BF16),
        grid_spec=pltpu.PrefetchScalarGridSpec(
            num_scalar_prefetch=1,
            grid=(1,),
            in_specs=[
                pl.BlockSpec((n, nbc), lambda i, c: (0, 0)),
                pl.BlockSpec((nbc, nbox), lambda i, c: (c[0], 0)),
            ],
            out_specs=pl.BlockSpec((n, nbox), lambda i, c: (0, 0)),
        ),
        compiler_params=params(),
        name="sphere_rows",
    )(column, onehot, coupling)


def couple_kernel(rows, sums, out):
    nbox = rows.shape[1]
    feat = sums.shape[2]
    n, sd = out.shape[0], out.shape[1]
    out[...] = dot(rows[...], sums[...].reshape(nbox, feat)).astype(BF16).reshape(n, sd, feat)


def couple(rows, sums, n, sd):
    return pl.pallas_call(
        couple_kernel,
        out_shape=jax.ShapeDtypeStruct((n, sd, sums.shape[2]), BF16),
        compiler_params=params(),
        name="couple",
    )(rows, sums)


def prep_kernel(counts, axial, rot, perm, permt, out_map, in_map, tmat, turn, scale, maps, tre, tim, cols):
    sd, slots, width = axial.shape
    n = width // 2
    turn[...] = jnp.zeros_like(turn)
    for k in range(slots):
        turn[k * LANES:k * LANES + width, :] = dot(rot[k], perm[...]).astype(BF16)
    slot = lax.broadcasted_iota(jnp.int32, (slots, LANES), 0)
    pad = jnp.zeros((slots, LANES - width), F32)
    for i in range(sd):
        factor = jnp.concatenate([axial[i].astype(F32), pad], axis=1)
        scale[pl.ds(i, slots, stride=sd), :] = jnp.where(slot < counts[i], factor, 0.0)
    both = dot(in_map[...], out_map[...])
    hi = both.astype(BF16)
    lo = (both - hi.astype(F32)).astype(BF16)
    for r, part in enumerate((hi, lo)):
        moved = dot(dot(permt[...], part).astype(BF16), perm[...])
        maps[r * LANES:r * LANES + HALF, :] = moved[:HALF].astype(BF16)
        maps[r * LANES + HALF:(r + 1) * LANES, :] = swap_halves(moved[HALF:]).astype(BF16)
    cols[...] = tmat[...].T
    lane = lax.broadcasted_iota(jnp.int32, (n, LANES), 1) < HALF
    even = cols[pl.ds(0, n, stride=2), :]
    odd = cols[pl.ds(1, n, stride=2), :]
    for i in range(sd):
        row = jnp.where(lane, even[:, i:i + 1], odd[:, i:i + 1])
        tre[i] = row[:n // 2]
        tim[i] = row[n // 2:]


def prepare(counts, axial, rot, perm, permt, out_map, in_map, tmat):
    sd, slots, width = axial.shape
    vmem = pl.BlockSpec(memory_space=pltpu.VMEM)
    spread = jax.ShapeDtypeStruct((sd, width // 4, LANES), F32)
    return pl.pallas_call(
        prep_kernel,
        out_shape=(
            jax.ShapeDtypeStruct((slots * LANES, LANES), BF16),
            jax.ShapeDtypeStruct((slots * sd, LANES), F32),
            jax.ShapeDtypeStruct((2 * LANES, LANES), BF16),
            spread,
            spread,
        ),
        in_specs=[pl.BlockSpec(memory_space=pltpu.SMEM)] + [vmem] * 7,
        scratch_shapes=[pltpu.VMEM((width, sd), F32)],
        compiler_params=params(),
        name="prepare",
    )(counts, axial, rot, perm, permt, out_map, in_map, tmat)


def near_kernel(nbr, column, side_a, own, side_b, scale, turn, out, sides, planes, cand, diag, total, sems):
    sd, slots = nbr.shape
    copies = [pltpu.make_async_copy(src, sides.at[n], sems.at[n]) for n, src in enumerate((side_a, side_b))]
    for copy in copies:
        copy.start()
    lane = lax.broadcasted_iota(jnp.int32, (HALF, LANES), 1) < HALF
    diag[...] = jnp.zeros_like(diag)
    planes[...] = jnp.zeros_like(planes)
    odd = column[0] % 2
    for c, base in ((1, sd), (0, 2 * sd * (1 - odd)), (2, 2 * sd * odd)):
        if c != 1:
            copies[c // 2].wait()
        to_planes(own if c == 1 else sides[c // 2], planes, 0)
        for s in range(0, sd, 2):
            both = planes[s * HALF:(s + 2) * HALF, :].T
            top, bottom = both[:HALF], both[HALF:]
            cand[base + s] = jnp.where(lane, top, swap_halves(bottom)).astype(BF16)
            cand[base + s + 1] = jnp.where(lane, swap_halves(top), bottom).astype(BF16)
    total[...] = jnp.zeros_like(total)
    group = 4

    def pair(q, diag):
        k = 2 * q
        r = pl.multiple_of(q * 2 * LANES, 2 * LANES)
        diag[:LANES, :LANES] = turn[pl.ds(r, LANES), :]
        diag[LANES:, LANES:] = turn[pl.ds(r + LANES, LANES), :]
        fact0 = scale[pl.ds(pl.multiple_of(k * sd, sd), sd), :]
        fact1 = scale[pl.ds(pl.multiple_of(k * sd + sd, sd), sd), :]
        back = turn[pl.ds(r, 2 * LANES), :]
        fwd = diag[...]
        for g in range(sd // group):
            picked = []
            for s in range(g * group, (g + 1) * group):
                a = cand[nbr[s, k]]
                b = cand[nbr[s, k + 1]]
                picked.append(jnp.concatenate([a, b], axis=1))
            turned = dot(jnp.concatenate(picked, axis=0), fwd, 1, 1)
            scaled = []
            for n, s in enumerate(range(g * group, (g + 1) * group)):
                f = jnp.concatenate([fact0[s:s + 1], fact1[s:s + 1]], axis=1)
                scaled.append((turned[n * HALF:(n + 1) * HALF] * f).astype(BF16))
            rows = pl.ds(g * group * HALF, group * HALF)
            total[rows, :] += dot(jnp.concatenate(scaled, axis=0), back)

    def step(m, carry):
        for u in range(UNROLL):
            pair(UNROLL * m + u, diag.at[u])
        return carry

    lax.fori_loop(0, slots // (2 * UNROLL), step, 0)
    for s in range(0, sd, 2):
        a = total[s * HALF:(s + 1) * HALF, :]
        b = total[(s + 1) * HALF:(s + 2) * HALF, :]
        top = jnp.where(lane, a, swap_halves(b))
        bottom = jnp.where(lane, swap_halves(a), b)
        out[s * HALF:(s + 2) * HALF, :] = jnp.concatenate([top, bottom], axis=0).T


def near_field(nbr, column, side_a, own, side_b, scale, turn):
    sd, _ = nbr.shape
    vmem = pl.BlockSpec(memory_space=pltpu.VMEM)
    place = pl.BlockSpec(memory_space=pl.ANY)
    return pl.pallas_call(
        near_kernel,
        out_shape=jax.ShapeDtypeStruct((sd * HALF, LANES), F32),
        in_specs=[pl.BlockSpec(memory_space=pltpu.SMEM)] * 2 + [place, vmem, place, vmem, vmem],
        out_specs=vmem,
        scratch_shapes=[
            pltpu.VMEM((2, *own.shape), BF16),
            pltpu.VMEM((sd * HALF, LANES), F32),
            pltpu.VMEM((3 * sd, HALF, LANES), BF16),
            pltpu.VMEM((UNROLL, 2 * LANES, 2 * LANES), BF16),
            pltpu.VMEM((sd * HALF, LANES), F32),
            pltpu.SemaphoreType.DMA((2,)),
        ],
        compiler_params=params(),
        name="near",
    )(nbr, column, side_a, own, side_b, scale, turn)


def tail_kernel(got, near, x, tmat_re, tmat_im, maps, out, planes):
    ngrp, sd, feat = got.shape
    per = feat // LANES
    lane = lax.broadcasted_iota(jnp.int32, (HALF, LANES), 1) < HALF
    half = tmat_re.shape[1]
    planes[...] = jnp.zeros_like(planes)
    for g in range(ngrp):
        part = got[g]
        for q in range(per):
            t = g * per + q
            planes[pl.ds(t, sd, stride=HALF), :] = part[:, q * LANES:(q + 1) * LANES].astype(F32)
    hi = maps[:LANES]
    lo = maps[LANES:]
    for s in range(sd):
        loc = planes[s * HALF:(s + 1) * HALF, :]
        both = jnp.concatenate([loc, swap_halves(loc)], axis=0).astype(BF16)
        prod = dot(hi, both) + dot(lo, both)
        field = near[s * HALF:(s + 1) * HALF, :] + jnp.where(lane, prod[:HALF], prod[HALF:])
        ur, ui = field[:half], field[half:2 * half]
        tr, ti = tmat_re[s], tmat_im[s]
        planes[s * HALF:s * HALF + half, :] = tr * ur - ti * ui
        planes[s * HALF + half:s * HALF + 2 * half, :] = tr * ui + ti * ur
    for t in range(2 * half):
        cols = slice(t * LANES, (t + 1) * LANES)
        out[:, cols] = (x[:, cols].astype(F32) - planes[pl.ds(t, sd, stride=HALF), :]).astype(BF16)


def tail(got, near, coeffs, tmat_re, tmat_im, maps):
    sd = coeffs.shape[0]
    return pl.pallas_call(
        tail_kernel,
        out_shape=jax.ShapeDtypeStruct(coeffs.shape, BF16),
        scratch_shapes=[pltpu.VMEM((sd * HALF, LANES), F32)],
        compiler_params=params(),
        name="tail",
    )(got, near, coeffs, tmat_re, tmat_im, maps)


def shards(coeffs, neighbours, counts, boxes, axial, rotations, out_map, coupling, in_map, tmat):
    sd, _ = coeffs.shape
    width = rotations.shape[1]
    ngrp = lax.axis_size("grp")
    ncell = lax.axis_size("cells")
    nbc = NBG * ngrp
    first = [p for i in range(0, ncell - 1, 2) for p in ((i, i + 1), (i + 1, i))]
    second = [p for i in range(1, ncell - 1, 2) for p in ((i, i + 1), (i + 1, i))]
    column = lax.axis_index("cells").astype(jnp.int32)[None]
    near_a = lax.ppermute(coeffs, "cells", first)
    near_b = lax.ppermute(coeffs, "cells", second)
    sent = pack(coeffs, boxes, ngrp)
    got = lax.all_to_all(sent, "grp", 0, 0, tiled=True)
    spot = jnp.arange(width, dtype=jnp.int32)
    spot = (spot % 2) * HALF + spot // 2
    lanes = jnp.arange(LANES, dtype=jnp.int32)
    perm = (spot[:, None] == lanes[None, :]).astype(BF16)
    permt = (lanes[:, None] == spot[None, :]).astype(BF16)
    turn, scale, maps, tre, tim = prepare(
        counts, axial, rotations, perm, permt, out_map, in_map, tmat
    )
    sums, onehot = box_sums(got, nbc, ncell)
    every = lax.all_to_all(sums, "cells", 0, 0, tiled=True)
    rows = sphere_rows(column, onehot, coupling)
    near = near_field(neighbours, column, near_a, coeffs, near_b, scale, turn)
    local = couple(rows, every, ngrp, sd)
    mine = lax.all_to_all(local, "grp", 0, 0, tiled=True)
    return tail(mine, near, coeffs, tre, tim, maps)


def solution(mesh):
    rows = P(("cells", "grp"), None)
    flat = P(("cells", "grp"))
    in_specs = (rows, rows, flat, flat, P(("cells", "grp"), None, None), P(), P(), P(), P(), rows)
    return jax.shard_map(shards, mesh=mesh, in_specs=in_specs, out_specs=rows, check_vma=False)
```

```python
import functools

import jax
import jax.numpy as jnp
from jax import lax
from jax.experimental import pallas as pl
from jax.experimental.pallas import tpu as pltpu
from jax.sharding import PartitionSpec as P


F32 = jnp.float32
BF16 = jnp.bfloat16
NBG = 2
LANES = 128
HALF = 64
UNROLL = 8


def dot(a, b, ca=1, cb=0):
    return lax.dot_general(a, b, (((ca,), (cb,)), ((), ())), preferred_element_type=F32)


def params():
    return pltpu.CompilerParams(vmem_limit_bytes=12 * 1024 * 1024)


def to_planes(rows, planes, base):
    sd, width = rows.shape
    for t in range(width // LANES):
        planes[pl.ds(base * HALF + t, sd, stride=HALF), :] = rows[:, t * LANES:(t + 1) * LANES].astype(F32)


def swap_halves(a):
    return pltpu.roll(a, HALF, 1)


def pack_kernel(boxes, x, out):
    ngrp, sd, wide = out.shape
    feat = wide - LANES
    row = lax.broadcasted_iota(jnp.int32, (sd, LANES), 0)
    mark = jnp.zeros((sd, LANES), F32)
    for s in range(sd):
        mark = jnp.where(row == s, boxes[s].astype(F32), mark)
    tag = mark.astype(BF16)
    for g in range(ngrp):
        out[g, :, :feat] = x[:, g * feat:(g + 1) * feat]
        out[g, :, feat:] = tag


def pack(coeffs, boxes, ngrp):
    sd, width = coeffs.shape
    vmem = pl.BlockSpec(memory_space=pltpu.VMEM)
    return pl.pallas_call(
        pack_kernel,
        out_shape=jax.ShapeDtypeStruct((ngrp, sd, width // ngrp + LANES), BF16),
        in_specs=[pl.BlockSpec(memory_space=pltpu.SMEM), vmem],
        out_specs=vmem,
        compiler_params=pltpu.CompilerParams(vmem_limit_bytes=62 * 1024 * 1024),
        name="pack",
    )(boxes, coeffs)


def sums_kernel(got, out, onehot, *, nbc):
    n, sd, wide = got.shape
    feat = wide - LANES
    flat = got[...].reshape(n * sd, wide)
    box = flat[:, feat:feat + nbc].astype(F32)
    ids = lax.broadcasted_iota(jnp.int32, (n * sd, nbc), 1).astype(F32)
    hot = (box == ids).astype(F32).astype(BF16)
    onehot[...] = hot
    sums = dot(hot, flat[:, :feat], 0, 0).astype(BF16)
    for c in range(out.shape[0]):
        out[c] = sums


def box_sums(got, nbc, ncell):
    n, sd, wide = got.shape
    return pl.pallas_call(
        functools.partial(sums_kernel, nbc=nbc),
        out_shape=(
            jax.ShapeDtypeStruct((ncell, nbc, wide - LANES), BF16),
            jax.ShapeDtypeStruct((n * sd, nbc), BF16),
        ),
        compiler_params=params(),
        name="box_sums",
    )(got)


def rows_kernel(column, onehot, coupling, out):
    out[...] = dot(onehot[...], coupling[...]).astype(BF16)


def sphere_rows(column, onehot, coupling):
    n, nbc = onehot.shape
    nbox = coupling.shape[1]
    return pl.pallas_call(
        rows_kernel,
        out_shape=jax.ShapeDtypeStruct((n, nbox), BF16),
        grid_spec=pltpu.PrefetchScalarGridSpec(
            num_scalar_prefetch=1,
            grid=(1,),
            in_specs=[
                pl.BlockSpec((n, nbc), lambda i, c: (0, 0)),
                pl.BlockSpec((nbc, nbox), lambda i, c: (c[0], 0)),
            ],
            out_specs=pl.BlockSpec((n, nbox), lambda i, c: (0, 0)),
        ),
        compiler_params=params(),
        name="sphere_rows",
    )(column, onehot, coupling)


def couple_kernel(rows, sums, out):
    nbox = rows.shape[1]
    feat = sums.shape[2]
    n, sd = out.shape[0], out.shape[1]
    out[...] = dot(rows[...], sums[...].reshape(nbox, feat)).astype(BF16).reshape(n, sd, feat)


def couple(rows, sums, n, sd):
    return pl.pallas_call(
        couple_kernel,
        out_shape=jax.ShapeDtypeStruct((n, sd, sums.shape[2]), BF16),
        compiler_params=params(),
        name="couple",
    )(rows, sums)


def prep_kernel(counts, axial, rot, perm, permt, out_map, in_map, tmat, turn, scale, maps, tre, tim, cols):
    sd, slots, width = axial.shape
    n = width // 2
    turn[...] = jnp.zeros_like(turn)
    for k in range(slots):
        turn[k * LANES:k * LANES + width, :] = dot(rot[k], perm[...]).astype(BF16)
    slot = lax.broadcasted_iota(jnp.int32, (slots, LANES), 0)
    pad = jnp.zeros((slots, LANES - width), F32)
    for i in range(sd):
        factor = jnp.concatenate([axial[i].astype(F32), pad], axis=1)
        scale[pl.ds(i, slots, stride=sd), :] = jnp.where(slot < counts[i], factor, 0.0)
    both = dot(in_map[...], out_map[...])
    hi = both.astype(BF16)
    lo = (both - hi.astype(F32)).astype(BF16)
    for r, part in enumerate((hi, lo)):
        moved = dot(dot(permt[...], part).astype(BF16), perm[...])
        maps[r * LANES:r * LANES + HALF, :] = moved[:HALF].astype(BF16)
        maps[r * LANES + HALF:(r + 1) * LANES, :] = swap_halves(moved[HALF:]).astype(BF16)
    cols[...] = tmat[...].T
    lane = lax.broadcasted_iota(jnp.int32, (n, LANES), 1) < HALF
    even = cols[pl.ds(0, n, stride=2), :]
    odd = cols[pl.ds(1, n, stride=2), :]
    for i in range(sd):
        row = jnp.where(lane, even[:, i:i + 1], odd[:, i:i + 1])
        tre[i] = row[:n // 2]
        tim[i] = row[n // 2:]


def prepare(counts, axial, rot, perm, permt, out_map, in_map, tmat):
    sd, slots, width = axial.shape
    vmem = pl.BlockSpec(memory_space=pltpu.VMEM)
    spread = jax.ShapeDtypeStruct((sd, width // 4, LANES), F32)
    return pl.pallas_call(
        prep_kernel,
        out_shape=(
            jax.ShapeDtypeStruct((slots * LANES, LANES), BF16),
            jax.ShapeDtypeStruct((slots * sd, LANES), F32),
            jax.ShapeDtypeStruct((2 * LANES, LANES), BF16),
            spread,
            spread,
        ),
        in_specs=[pl.BlockSpec(memory_space=pltpu.SMEM)] + [vmem] * 7,
        scratch_shapes=[pltpu.VMEM((width, sd), F32)],
        compiler_params=params(),
        name="prepare",
    )(counts, axial, rot, perm, permt, out_map, in_map, tmat)


def near_kernel(nbr, column, side_a, own, side_b, scale, turn, out, sides, planes, cand, diag, total, sems):
    sd, slots = nbr.shape
    copies = [pltpu.make_async_copy(src, sides.at[n], sems.at[n]) for n, src in enumerate((side_a, side_b))]
    for copy in copies:
        copy.start()
    lane = lax.broadcasted_iota(jnp.int32, (HALF, LANES), 1) < HALF
    diag[...] = jnp.zeros_like(diag)
    planes[...] = jnp.zeros_like(planes)
    odd = column[0] % 2
    for c, base in ((1, sd), (0, 2 * sd * (1 - odd)), (2, 2 * sd * odd)):
        if c != 1:
            copies[c // 2].wait()
        to_planes(own if c == 1 else sides[c // 2], planes, 0)
        for s in range(0, sd, 2):
            both = planes[s * HALF:(s + 2) * HALF, :].T
            top, bottom = both[:HALF], both[HALF:]
            cand[base + s] = jnp.where(lane, top, swap_halves(bottom)).astype(BF16)
            cand[base + s + 1] = jnp.where(lane, swap_halves(top), bottom).astype(BF16)
    total[...] = jnp.zeros_like(total)
    group = 4

    def pair(q, diag):
        k = 2 * q
        r = pl.multiple_of(q * 2 * LANES, 2 * LANES)
        diag[:LANES, :LANES] = turn[pl.ds(r, LANES), :]
        diag[LANES:, LANES:] = turn[pl.ds(r + LANES, LANES), :]
        fact0 = scale[pl.ds(pl.multiple_of(k * sd, sd), sd), :]
        fact1 = scale[pl.ds(pl.multiple_of(k * sd + sd, sd), sd), :]
        back = turn[pl.ds(r, 2 * LANES), :]
        fwd = diag[...]
        for g in range(sd // group):
            picked = []
            for s in range(g * group, (g + 1) * group):
                a = cand[nbr[s, k]]
                b = cand[nbr[s, k + 1]]
                picked.append(jnp.concatenate([a, b], axis=1))
            turned = dot(jnp.concatenate(picked, axis=0), fwd, 1, 1)
            scaled = []
            for n, s in enumerate(range(g * group, (g + 1) * group)):
                f = jnp.concatenate([fact0[s:s + 1], fact1[s:s + 1]], axis=1)
                scaled.append((turned[n * HALF:(n + 1) * HALF] * f).astype(BF16))
            rows = pl.ds(g * group * HALF, group * HALF)
            total[rows, :] += dot(jnp.concatenate(scaled, axis=0), back)

    def step(m, carry):
        for u in range(UNROLL):
            pair(UNROLL * m + u, diag.at[u])
        return carry

    lax.fori_loop(0, slots // (2 * UNROLL), step, 0)
    for s in range(0, sd, 2):
        a = total[s * HALF:(s + 1) * HALF, :]
        b = total[(s + 1) * HALF:(s + 2) * HALF, :]
        top = jnp.where(lane, a, swap_halves(b))
        bottom = jnp.where(lane, swap_halves(a), b)
        out[s * HALF:(s + 2) * HALF, :] = jnp.concatenate([top, bottom], axis=0).T


def near_field(nbr, column, side_a, own, side_b, scale, turn):
    sd, _ = nbr.shape
    vmem = pl.BlockSpec(memory_space=pltpu.VMEM)
    place = pl.BlockSpec(memory_space=pl.ANY)
    return pl.pallas_call(
        near_kernel,
        out_shape=jax.ShapeDtypeStruct((sd * HALF, LANES), F32),
        in_specs=[pl.BlockSpec(memory_space=pltpu.SMEM)] * 2 + [place, vmem, place, vmem, vmem],
        out_specs=vmem,
        scratch_shapes=[
            pltpu.VMEM((2, *own.shape), BF16),
            pltpu.VMEM((sd * HALF, LANES), F32),
            pltpu.VMEM((3 * sd, HALF, LANES), BF16),
            pltpu.VMEM((UNROLL, 2 * LANES, 2 * LANES), BF16),
            pltpu.VMEM((sd * HALF, LANES), F32),
            pltpu.SemaphoreType.DMA((2,)),
        ],
        compiler_params=params(),
        name="near",
    )(nbr, column, side_a, own, side_b, scale, turn)


def tail_kernel(got, near, x, tmat_re, tmat_im, maps, out, planes):
    ngrp, sd, feat = got.shape
    per = feat // LANES
    lane = lax.broadcasted_iota(jnp.int32, (HALF, LANES), 1) < HALF
    half = tmat_re.shape[1]
    planes[...] = jnp.zeros_like(planes)
    for g in range(ngrp):
        part = got[g]
        for q in range(per):
            t = g * per + q
            planes[pl.ds(t, sd, stride=HALF), :] = part[:, q * LANES:(q + 1) * LANES].astype(F32)
    hi = maps[:LANES]
    lo = maps[LANES:]
    for s in range(sd):
        loc = planes[s * HALF:(s + 1) * HALF, :]
        both = jnp.concatenate([loc, swap_halves(loc)], axis=0).astype(BF16)
        prod = dot(hi, both) + dot(lo, both)
        field = near[s * HALF:(s + 1) * HALF, :] + jnp.where(lane, prod[:HALF], prod[HALF:])
        ur, ui = field[:half], field[half:2 * half]
        tr, ti = tmat_re[s], tmat_im[s]
        planes[s * HALF:s * HALF + half, :] = tr * ur - ti * ui
        planes[s * HALF + half:s * HALF + 2 * half, :] = tr * ui + ti * ur
    for t in range(2 * half):
        cols = slice(t * LANES, (t + 1) * LANES)
        out[:, cols] = (x[:, cols].astype(F32) - planes[pl.ds(t, sd, stride=HALF), :]).astype(BF16)


def tail(got, near, coeffs, tmat_re, tmat_im, maps):
    sd = coeffs.shape[0]
    return pl.pallas_call(
        tail_kernel,
        out_shape=jax.ShapeDtypeStruct(coeffs.shape, BF16),
        scratch_shapes=[pltpu.VMEM((sd * HALF, LANES), F32)],
        compiler_params=params(),
        name="tail",
    )(got, near, coeffs, tmat_re, tmat_im, maps)


def shards(coeffs, neighbours, counts, boxes, axial, rotations, out_map, coupling, in_map, tmat):
    sd, _ = coeffs.shape
    width = rotations.shape[1]
    ngrp = lax.axis_size("grp")
    ncell = lax.axis_size("cells")
    nbc = NBG * ngrp
    first = [p for i in range(0, ncell - 1, 2) for p in ((i, i + 1), (i + 1, i))]
    second = [p for i in range(1, ncell - 1, 2) for p in ((i, i + 1), (i + 1, i))]
    column = lax.axis_index("cells").astype(jnp.int32)[None]
    near_a = lax.ppermute(coeffs, "cells", first)
    near_b = lax.ppermute(coeffs, "cells", second)
    sent = pack(coeffs, boxes, ngrp)
    got = lax.all_to_all(sent, "grp", 0, 0, tiled=True)
    spot = jnp.arange(width, dtype=jnp.int32)
    spot = (spot % 2) * HALF + spot // 2
    lanes = jnp.arange(LANES, dtype=jnp.int32)
    perm = (spot[:, None] == lanes[None, :]).astype(BF16)
    permt = (lanes[:, None] == spot[None, :]).astype(BF16)
    turn, scale, maps, tre, tim = prepare(
        counts, axial, rotations, perm, permt, out_map, in_map, tmat
    )
    sums, onehot = box_sums(got, nbc, ncell)
    every = lax.all_to_all(sums, "cells", 0, 0, tiled=True)
    rows = sphere_rows(column, onehot, coupling)
    near = near_field(neighbours, column, near_a, coeffs, near_b, scale, turn)
    local = couple(rows, every, ngrp, sd)
    mine = lax.all_to_all(local, "grp", 0, 0, tiled=True)
    return tail(mine, near, coeffs, tre, tim, maps)


def solution(mesh):
    rows = P(("cells", "grp"), None)
    flat = P(("cells", "grp"))
    in_specs = (rows, rows, flat, flat, P(("cells", "grp"), None, None), P(), P(), P(), P(), rows)
    return jax.shard_map(shards, mesh=mesh, in_specs=in_specs, out_specs=rows, check_vma=False)
```

```python
import functools

import jax
import jax.numpy as jnp
from jax import lax
from jax.experimental import pallas as pl
from jax.experimental.pallas import tpu as pltpu
from jax.sharding import PartitionSpec as P


F32 = jnp.float32
BF16 = jnp.bfloat16
NBG = 2
LANES = 128
HALF = 64
PITCH = 72
UNROLL = 8


def dot(a, b, ca=1, cb=0):
    return lax.dot_general(a, b, (((ca,), (cb,)), ((), ())), preferred_element_type=F32)


def params():
    return pltpu.CompilerParams(vmem_limit_bytes=12 * 1024 * 1024)


def to_planes(rows, planes, base):
    sd, width = rows.shape
    for t in range(width // LANES):
        planes[pl.ds(base * PITCH + t, sd, stride=PITCH), :] = rows[:, t * LANES:(t + 1) * LANES].astype(F32)


def swap_halves(a):
    return pltpu.roll(a, HALF, 1)


def pack_kernel(boxes, x, out):
    ngrp, sd, wide = out.shape
    feat = wide - LANES
    row = lax.broadcasted_iota(jnp.int32, (sd, LANES), 0)
    mark = jnp.zeros((sd, LANES), F32)
    for s in range(sd):
        mark = jnp.where(row == s, boxes[s].astype(F32), mark)
    tag = mark.astype(BF16)
    for g in range(ngrp):
        out[g, :, :feat] = x[:, g * feat:(g + 1) * feat]
        out[g, :, feat:] = tag


def pack(coeffs, boxes, ngrp):
    sd, width = coeffs.shape
    vmem = pl.BlockSpec(memory_space=pltpu.VMEM)
    return pl.pallas_call(
        pack_kernel,
        out_shape=jax.ShapeDtypeStruct((ngrp, sd, width // ngrp + LANES), BF16),
        in_specs=[pl.BlockSpec(memory_space=pltpu.SMEM), vmem],
        out_specs=vmem,
        compiler_params=pltpu.CompilerParams(vmem_limit_bytes=62 * 1024 * 1024),
        name="pack",
    )(boxes, coeffs)


def sums_kernel(got, out, onehot, *, nbc):
    n, sd, wide = got.shape
    feat = wide - LANES
    flat = got[...].reshape(n * sd, wide)
    box = flat[:, feat:feat + nbc].astype(F32)
    ids = lax.broadcasted_iota(jnp.int32, (n * sd, nbc), 1).astype(F32)
    hot = (box == ids).astype(F32).astype(BF16)
    onehot[...] = hot
    sums = dot(hot, flat[:, :feat], 0, 0).astype(BF16)
    for c in range(out.shape[0]):
        out[c] = sums


def box_sums(got, nbc, ncell):
    n, sd, wide = got.shape
    return pl.pallas_call(
        functools.partial(sums_kernel, nbc=nbc),
        out_shape=(
            jax.ShapeDtypeStruct((ncell, nbc, wide - LANES), BF16),
            jax.ShapeDtypeStruct((n * sd, nbc), BF16),
        ),
        compiler_params=params(),
        name="box_sums",
    )(got)


def rows_kernel(column, onehot, coupling, out):
    out[...] = dot(onehot[...], coupling[...]).astype(BF16)


def sphere_rows(column, onehot, coupling):
    n, nbc = onehot.shape
    nbox = coupling.shape[1]
    return pl.pallas_call(
        rows_kernel,
        out_shape=jax.ShapeDtypeStruct((n, nbox), BF16),
        grid_spec=pltpu.PrefetchScalarGridSpec(
            num_scalar_prefetch=1,
            grid=(1,),
            in_specs=[
                pl.BlockSpec((n, nbc), lambda i, c: (0, 0)),
                pl.BlockSpec((nbc, nbox), lambda i, c: (c[0], 0)),
            ],
            out_specs=pl.BlockSpec((n, nbox), lambda i, c: (0, 0)),
        ),
        compiler_params=params(),
        name="sphere_rows",
    )(column, onehot, coupling)


def couple_kernel(rows, sums, out):
    nbox = rows.shape[1]
    feat = sums.shape[2]
    n, sd = out.shape[0], out.shape[1]
    out[...] = dot(rows[...], sums[...].reshape(nbox, feat)).astype(BF16).reshape(n, sd, feat)


def couple(rows, sums, n, sd):
    return pl.pallas_call(
        couple_kernel,
        out_shape=jax.ShapeDtypeStruct((n, sd, sums.shape[2]), BF16),
        compiler_params=params(),
        name="couple",
    )(rows, sums)


def prep_kernel(counts, axial, rot, perm, permt, out_map, in_map, tmat, turn, scale, maps, tre, tim, cols):
    sd, slots, width = axial.shape
    n = width // 2
    turn[...] = jnp.zeros_like(turn)
    for k in range(slots):
        turn[k * LANES:k * LANES + width, :] = dot(rot[k], perm[...]).astype(BF16)
    slot = lax.broadcasted_iota(jnp.int32, (slots, LANES), 0)
    pad = jnp.zeros((slots, LANES - width), F32)
    for i in range(sd):
        factor = jnp.concatenate([axial[i].astype(F32), pad], axis=1)
        scale[pl.ds(i, slots, stride=sd), :] = jnp.where(slot < counts[i], factor, 0.0)
    both = dot(in_map[...], out_map[...])
    hi = both.astype(BF16)
    lo = (both - hi.astype(F32)).astype(BF16)
    for r, part in enumerate((hi, lo)):
        moved = dot(dot(permt[...], part).astype(BF16), perm[...])
        maps[r * LANES:r * LANES + HALF, :] = moved[:HALF].astype(BF16)
        maps[r * LANES + HALF:(r + 1) * LANES, :] = swap_halves(moved[HALF:]).astype(BF16)
    cols[...] = tmat[...].T
    lane = lax.broadcasted_iota(jnp.int32, (n, LANES), 1) < HALF
    even = cols[pl.ds(0, n, stride=2), :]
    odd = cols[pl.ds(1, n, stride=2), :]
    for i in range(sd):
        row = jnp.where(lane, even[:, i:i + 1], odd[:, i:i + 1])
        tre[i] = row[:n // 2]
        tim[i] = row[n // 2:]


def prepare(counts, axial, rot, perm, permt, out_map, in_map, tmat):
    sd, slots, width = axial.shape
    vmem = pl.BlockSpec(memory_space=pltpu.VMEM)
    spread = jax.ShapeDtypeStruct((sd, width // 4, LANES), F32)
    return pl.pallas_call(
        prep_kernel,
        out_shape=(
            jax.ShapeDtypeStruct((slots * LANES, LANES), BF16),
            jax.ShapeDtypeStruct((slots * sd, LANES), F32),
            jax.ShapeDtypeStruct((2 * LANES, LANES), BF16),
            spread,
            spread,
        ),
        in_specs=[pl.BlockSpec(memory_space=pltpu.SMEM)] + [vmem] * 7,
        scratch_shapes=[pltpu.VMEM((width, sd), F32)],
        compiler_params=params(),
        name="prepare",
    )(counts, axial, rot, perm, permt, out_map, in_map, tmat)


def near_kernel(nbr, column, side_a, own, side_b, scale, turn, out, sides, planes, cand, diag, total, sems):
    sd, slots = nbr.shape
    copies = [pltpu.make_async_copy(src, sides.at[n], sems.at[n]) for n, src in enumerate((side_a, side_b))]
    for copy in copies:
        copy.start()
    lane = lax.broadcasted_iota(jnp.int32, (HALF, LANES), 1) < HALF
    diag[...] = jnp.zeros_like(diag)
    planes[...] = jnp.zeros_like(planes)
    odd = column[0] % 2
    for c, base in ((1, sd), (0, 2 * sd * (1 - odd)), (2, 2 * sd * odd)):
        if c != 1:
            copies[c // 2].wait()
        to_planes(own if c == 1 else sides[c // 2], planes, 0)
        for s in range(0, sd, 2):
            both = jnp.concatenate(
                [planes[r * PITCH:r * PITCH + HALF, :] for r in (s, s + 1)], axis=0
            ).T
            top, bottom = both[:HALF], both[HALF:]
            cand[base + s] = jnp.where(lane, top, swap_halves(bottom)).astype(BF16)
            cand[base + s + 1] = jnp.where(lane, swap_halves(top), bottom).astype(BF16)
    total[...] = jnp.zeros_like(total)
    group = 4

    def pair(q, diag):
        k = 2 * q
        r = pl.multiple_of(q * 2 * LANES, 2 * LANES)
        diag[:LANES, :LANES] = turn[pl.ds(r, LANES), :]
        diag[LANES:, LANES:] = turn[pl.ds(r + LANES, LANES), :]
        fact0 = scale[pl.ds(pl.multiple_of(k * sd, sd), sd), :]
        fact1 = scale[pl.ds(pl.multiple_of(k * sd + sd, sd), sd), :]
        back = turn[pl.ds(r, 2 * LANES), :]
        fwd = diag[...]
        for g in range(sd // group):
            picked = []
            for s in range(g * group, (g + 1) * group):
                a = cand[nbr[s, k]]
                b = cand[nbr[s, k + 1]]
                picked.append(jnp.concatenate([a, b], axis=1))
            turned = dot(jnp.concatenate(picked, axis=0), fwd, 1, 1)
            scaled = []
            for n, s in enumerate(range(g * group, (g + 1) * group)):
                f = jnp.concatenate([fact0[s:s + 1], fact1[s:s + 1]], axis=1)
                scaled.append((turned[n * HALF:(n + 1) * HALF] * f).astype(BF16))
            rows = pl.ds(g * group * HALF, group * HALF)
            total[rows, :] += dot(jnp.concatenate(scaled, axis=0), back)

    def step(m, carry):
        for u in range(UNROLL):
            pair(UNROLL * m + u, diag.at[u])
        return carry

    lax.fori_loop(0, slots // (2 * UNROLL), step, 0)
    for s in range(0, sd, 2):
        a = total[s * HALF:(s + 1) * HALF, :]
        b = total[(s + 1) * HALF:(s + 2) * HALF, :]
        top = jnp.where(lane, a, swap_halves(b))
        bottom = jnp.where(lane, swap_halves(a), b)
        out[s * HALF:(s + 2) * HALF, :] = jnp.concatenate([top, bottom], axis=0).T


def near_field(nbr, column, side_a, own, side_b, scale, turn):
    sd, _ = nbr.shape
    vmem = pl.BlockSpec(memory_space=pltpu.VMEM)
    place = pl.BlockSpec(memory_space=pl.ANY)
    return pl.pallas_call(
        near_kernel,
        out_shape=jax.ShapeDtypeStruct((sd * HALF, LANES), F32),
        in_specs=[pl.BlockSpec(memory_space=pltpu.SMEM)] * 2 + [place, vmem, place, vmem, vmem],
        out_specs=vmem,
        scratch_shapes=[
            pltpu.VMEM((2, *own.shape), BF16),
            pltpu.VMEM((sd * PITCH, LANES), F32),
            pltpu.VMEM((3 * sd, HALF, LANES), BF16),
            pltpu.VMEM((UNROLL, 2 * LANES, 2 * LANES), BF16),
            pltpu.VMEM((sd * HALF, LANES), F32),
            pltpu.SemaphoreType.DMA((2,)),
        ],
        compiler_params=params(),
        name="near",
    )(nbr, column, side_a, own, side_b, scale, turn)


def tail_kernel(got, near, x, tmat_re, tmat_im, maps, out, planes):
    ngrp, sd, feat = got.shape
    per = feat // LANES
    lane = lax.broadcasted_iota(jnp.int32, (HALF, LANES), 1) < HALF
    half = tmat_re.shape[1]
    planes[...] = jnp.zeros_like(planes)
    for g in range(ngrp):
        part = got[g]
        for q in range(per):
            t = g * per + q
            planes[pl.ds(t, sd, stride=PITCH), :] = part[:, q * LANES:(q + 1) * LANES].astype(F32)
    hi = maps[:LANES]
    lo = maps[LANES:]
    for s in range(sd):
        loc = planes[s * PITCH:s * PITCH + HALF, :]
        both = jnp.concatenate([loc, swap_halves(loc)], axis=0).astype(BF16)
        prod = dot(hi, both) + dot(lo, both)
        field = near[s * HALF:(s + 1) * HALF, :] + jnp.where(lane, prod[:HALF], prod[HALF:])
        ur, ui = field[:half], field[half:2 * half]
        tr, ti = tmat_re[s], tmat_im[s]
        planes[s * PITCH:s * PITCH + half, :] = tr * ur - ti * ui
        planes[s * PITCH + half:s * PITCH + 2 * half, :] = tr * ui + ti * ur
    for t in range(2 * half):
        cols = slice(t * LANES, (t + 1) * LANES)
        out[:, cols] = (x[:, cols].astype(F32) - planes[pl.ds(t, sd, stride=PITCH), :]).astype(BF16)


def tail(got, near, coeffs, tmat_re, tmat_im, maps):
    sd = coeffs.shape[0]
    return pl.pallas_call(
        tail_kernel,
        out_shape=jax.ShapeDtypeStruct(coeffs.shape, BF16),
        scratch_shapes=[pltpu.VMEM((sd * PITCH, LANES), F32)],
        compiler_params=params(),
        name="tail",
    )(got, near, coeffs, tmat_re, tmat_im, maps)


def shards(coeffs, neighbours, counts, boxes, axial, rotations, out_map, coupling, in_map, tmat):
    sd, _ = coeffs.shape
    width = rotations.shape[1]
    ngrp = lax.axis_size("grp")
    ncell = lax.axis_size("cells")
    nbc = NBG * ngrp
    first = [p for i in range(0, ncell - 1, 2) for p in ((i, i + 1), (i + 1, i))]
    second = [p for i in range(1, ncell - 1, 2) for p in ((i, i + 1), (i + 1, i))]
    column = lax.axis_index("cells").astype(jnp.int32)[None]
    near_a = lax.ppermute(coeffs, "cells", first)
    near_b = lax.ppermute(coeffs, "cells", second)
    sent = pack(coeffs, boxes, ngrp)
    got = lax.all_to_all(sent, "grp", 0, 0, tiled=True)
    spot = jnp.arange(width, dtype=jnp.int32)
    spot = (spot % 2) * HALF + spot // 2
    lanes = jnp.arange(LANES, dtype=jnp.int32)
    perm = (spot[:, None] == lanes[None, :]).astype(BF16)
    permt = (lanes[:, None] == spot[None, :]).astype(BF16)
    turn, scale, maps, tre, tim = prepare(
        counts, axial, rotations, perm, permt, out_map, in_map, tmat
    )
    sums, onehot = box_sums(got, nbc, ncell)
    every = lax.all_to_all(sums, "cells", 0, 0, tiled=True)
    rows = sphere_rows(column, onehot, coupling)
    near = near_field(neighbours, column, near_a, coeffs, near_b, scale, turn)
    local = couple(rows, every, ngrp, sd)
    mine = lax.all_to_all(local, "grp", 0, 0, tiled=True)
    return tail(mine, near, coeffs, tre, tim, maps)


def solution(mesh):
    rows = P(("cells", "grp"), None)
    flat = P(("cells", "grp"))
    in_specs = (rows, rows, flat, flat, P(("cells", "grp"), None, None), P(), P(), P(), P(), rows)
    return jax.shard_map(shards, mesh=mesh, in_specs=in_specs, out_specs=rows, check_vma=False)
```

```python
import functools

import jax
import jax.numpy as jnp
from jax import lax
from jax.experimental import pallas as pl
from jax.experimental.pallas import tpu as pltpu
from jax.sharding import PartitionSpec as P


F32 = jnp.float32
BF16 = jnp.bfloat16
NBG = 2
LANES = 128
HALF = 64
PITCH = 72
UNROLL = 8
PARTS = 4


def dot(a, b, ca=1, cb=0):
    return lax.dot_general(a, b, (((ca,), (cb,)), ((), ())), preferred_element_type=F32)


def params():
    return pltpu.CompilerParams(vmem_limit_bytes=12 * 1024 * 1024)


def to_planes(rows, planes, base):
    sd, width = rows.shape
    for t in range(width // LANES):
        planes[pl.ds(base * PITCH + t, sd, stride=PITCH), :] = rows[:, t * LANES:(t + 1) * LANES].astype(F32)


def swap_halves(a):
    return pltpu.roll(a, HALF, 1)


def pack_kernel(boxes, x, out):
    ngrp, sd, wide = out.shape
    feat = wide - LANES
    row = lax.broadcasted_iota(jnp.int32, (sd, LANES), 0)
    mark = jnp.zeros((sd, LANES), F32)
    for s in range(sd):
        mark = jnp.where(row == s, boxes[s].astype(F32), mark)
    tag = mark.astype(BF16)
    for g in range(ngrp):
        out[g, :, :feat] = x[:, g * feat:(g + 1) * feat]
        out[g, :, feat:] = tag


def pack(coeffs, boxes, ngrp):
    sd, width = coeffs.shape
    vmem = pl.BlockSpec(memory_space=pltpu.VMEM)
    return pl.pallas_call(
        pack_kernel,
        out_shape=jax.ShapeDtypeStruct((ngrp, sd, width // ngrp + LANES), BF16),
        in_specs=[pl.BlockSpec(memory_space=pltpu.SMEM), vmem],
        out_specs=vmem,
        compiler_params=pltpu.CompilerParams(vmem_limit_bytes=62 * 1024 * 1024),
        name="pack",
    )(boxes, coeffs)


def sums_kernel(got, out, onehot, *, nbc):
    n, sd, wide = got.shape
    feat = wide - LANES
    flat = got[...].reshape(n * sd, wide)
    box = flat[:, feat:feat + nbc].astype(F32)
    ids = lax.broadcasted_iota(jnp.int32, (n * sd, nbc), 1).astype(F32)
    hot = (box == ids).astype(F32).astype(BF16)
    onehot[...] = hot
    sums = dot(hot, flat[:, :feat], 0, 0).astype(BF16)
    for c in range(out.shape[0]):
        out[c] = sums


def box_sums(got, nbc, ncell):
    n, sd, wide = got.shape
    return pl.pallas_call(
        functools.partial(sums_kernel, nbc=nbc),
        out_shape=(
            jax.ShapeDtypeStruct((ncell, nbc, wide - LANES), BF16),
            jax.ShapeDtypeStruct((n * sd, nbc), BF16),
        ),
        compiler_params=params(),
        name="box_sums",
    )(got)


def rows_kernel(column, onehot, coupling, out):
    out[...] = dot(onehot[...], coupling[...]).astype(BF16)


def sphere_rows(column, onehot, coupling):
    n, nbc = onehot.shape
    nbox = coupling.shape[1]
    return pl.pallas_call(
        rows_kernel,
        out_shape=jax.ShapeDtypeStruct((n, nbox), BF16),
        grid_spec=pltpu.PrefetchScalarGridSpec(
            num_scalar_prefetch=1,
            grid=(1,),
            in_specs=[
                pl.BlockSpec((n, nbc), lambda i, c: (0, 0)),
                pl.BlockSpec((nbc, nbox), lambda i, c: (c[0], 0)),
            ],
            out_specs=pl.BlockSpec((n, nbox), lambda i, c: (0, 0)),
        ),
        compiler_params=params(),
        name="sphere_rows",
    )(column, onehot, coupling)


def couple_kernel(rows, sums, out):
    nbox = rows.shape[1]
    feat = sums.shape[2]
    n, sd = out.shape[0], out.shape[1]
    out[...] = dot(rows[...], sums[...].reshape(nbox, feat)).astype(BF16).reshape(n, sd, feat)


def couple(rows, sums, n, sd):
    return pl.pallas_call(
        couple_kernel,
        out_shape=jax.ShapeDtypeStruct((n, sd, sums.shape[2]), BF16),
        compiler_params=params(),
        name="couple",
    )(rows, sums)


def prep_kernel(counts, axial, rot, perm, permt, out_map, in_map, tmat, turn, scale, maps, tre, tim, cols):
    sd, slots, width = axial.shape
    n = width // 2
    turn[...] = jnp.zeros_like(turn)
    for k in range(slots):
        turn[k * LANES:k * LANES + width, :] = dot(rot[k], perm[...]).astype(BF16)
    slot = lax.broadcasted_iota(jnp.int32, (slots, LANES), 0)
    pad = jnp.zeros((slots, LANES - width), F32)
    for i in range(sd):
        factor = jnp.concatenate([axial[i].astype(F32), pad], axis=1)
        scale[pl.ds(i, slots, stride=sd), :] = jnp.where(slot < counts[i], factor, 0.0)
    both = dot(in_map[...], out_map[...])
    hi = both.astype(BF16)
    lo = (both - hi.astype(F32)).astype(BF16)
    for r, part in enumerate((hi, lo)):
        moved = dot(dot(permt[...], part).astype(BF16), perm[...])
        maps[r * LANES:r * LANES + HALF, :] = moved[:HALF].astype(BF16)
        maps[r * LANES + HALF:(r + 1) * LANES, :] = swap_halves(moved[HALF:]).astype(BF16)
    cols[...] = tmat[...].T
    lane = lax.broadcasted_iota(jnp.int32, (n, LANES), 1) < HALF
    even = cols[pl.ds(0, n, stride=2), :]
    odd = cols[pl.ds(1, n, stride=2), :]
    for i in range(sd):
        row = jnp.where(lane, even[:, i:i + 1], odd[:, i:i + 1])
        tre[i] = row[:n // 2]
        tim[i] = row[n // 2:]


def prepare(counts, axial, rot, perm, permt, out_map, in_map, tmat):
    sd, slots, width = axial.shape
    vmem = pl.BlockSpec(memory_space=pltpu.VMEM)
    spread = jax.ShapeDtypeStruct((sd, width // 4, LANES), F32)
    return pl.pallas_call(
        prep_kernel,
        out_shape=(
            jax.ShapeDtypeStruct((slots * LANES, LANES), BF16),
            jax.ShapeDtypeStruct((slots * sd, LANES), F32),
            jax.ShapeDtypeStruct((2 * LANES, LANES), BF16),
            spread,
            spread,
        ),
        in_specs=[pl.BlockSpec(memory_space=pltpu.SMEM)] + [vmem] * 7,
        scratch_shapes=[pltpu.VMEM((width, sd), F32)],
        compiler_params=params(),
        name="prepare",
    )(counts, axial, rot, perm, permt, out_map, in_map, tmat)


def near_kernel(nbr, column, side_a, own, side_b, scale, turn, out, sides, planes, cand, diag, total, sems):
    sd, slots = nbr.shape
    copies = [pltpu.make_async_copy(src, sides.at[n], sems.at[n]) for n, src in enumerate((side_a, side_b))]
    for copy in copies:
        copy.start()
    lane = lax.broadcasted_iota(jnp.int32, (HALF, LANES), 1) < HALF
    diag[...] = jnp.zeros_like(diag)
    planes[...] = jnp.zeros_like(planes)
    odd = column[0] % 2
    for c, base in ((1, sd), (0, 2 * sd * (1 - odd)), (2, 2 * sd * odd)):
        if c != 1:
            copies[c // 2].wait()
        to_planes(own if c == 1 else sides[c // 2], planes, 0)
        for s in range(0, sd, 2):
            both = jnp.concatenate(
                [planes[r * PITCH:r * PITCH + HALF, :] for r in (s, s + 1)], axis=0
            ).T
            top, bottom = both[:HALF], both[HALF:]
            cand[base + s] = jnp.where(lane, top, swap_halves(bottom)).astype(BF16)
            cand[base + s + 1] = jnp.where(lane, swap_halves(top), bottom).astype(BF16)
    total[...] = jnp.zeros_like(total)
    group = 4

    def pair(q, diag):
        k = 2 * q
        r = pl.multiple_of(q * 2 * LANES, 2 * LANES)
        diag[:LANES, :LANES] = turn[pl.ds(r, LANES), :]
        diag[LANES:, LANES:] = turn[pl.ds(r + LANES, LANES), :]
        fact0 = scale[pl.ds(pl.multiple_of(k * sd, sd), sd), :]
        fact1 = scale[pl.ds(pl.multiple_of(k * sd + sd, sd), sd), :]
        back = turn[pl.ds(r, 2 * LANES), :]
        fwd = diag[...]
        for g in range(sd // group):
            picked = []
            for s in range(g * group, (g + 1) * group):
                a = cand[nbr[s, k]]
                b = cand[nbr[s, k + 1]]
                picked.append(jnp.concatenate([a, b], axis=1))
            turned = dot(jnp.concatenate(picked, axis=0), fwd, 1, 1)
            scaled = []
            for n, s in enumerate(range(g * group, (g + 1) * group)):
                f = jnp.concatenate([fact0[s:s + 1], fact1[s:s + 1]], axis=1)
                scaled.append((turned[n * HALF:(n + 1) * HALF] * f).astype(BF16))
            rows = pl.ds(g * group * HALF, group * HALF)
            total[rows, :] += dot(jnp.concatenate(scaled, axis=0), back)

    def step(m, carry):
        for u in range(UNROLL):
            pair(UNROLL * m + u, diag.at[u])
        return carry

    lax.fori_loop(0, slots // (2 * UNROLL), step, 0)
    for s in range(0, sd, 2):
        a = total[s * HALF:(s + 1) * HALF, :]
        b = total[(s + 1) * HALF:(s + 2) * HALF, :]
        top = jnp.where(lane, a, swap_halves(b))
        bottom = jnp.where(lane, swap_halves(a), b)
        out[s * HALF:(s + 2) * HALF, :] = jnp.concatenate([top, bottom], axis=0).T


def near_field(nbr, column, side_a, own, side_b, scale, turn):
    sd, _ = nbr.shape
    vmem = pl.BlockSpec(memory_space=pltpu.VMEM)
    place = pl.BlockSpec(memory_space=pl.ANY)
    return pl.pallas_call(
        near_kernel,
        out_shape=jax.ShapeDtypeStruct((sd * HALF, LANES), F32),
        in_specs=[pl.BlockSpec(memory_space=pltpu.SMEM)] * 2 + [place, vmem, place, vmem, vmem],
        out_specs=vmem,
        scratch_shapes=[
            pltpu.VMEM((2, *own.shape), BF16),
            pltpu.VMEM((sd * PITCH, LANES), F32),
            pltpu.VMEM((3 * sd, HALF, LANES), BF16),
            pltpu.VMEM((UNROLL, 2 * LANES, 2 * LANES), BF16),
            pltpu.VMEM((sd * HALF, LANES), F32),
            pltpu.SemaphoreType.DMA((2,)),
        ],
        compiler_params=params(),
        name="near",
    )(nbr, column, side_a, own, side_b, scale, turn)


def tail_kernel(got, near, x, tmat_re, tmat_im, maps, out, planes, ready, sems):
    ngrp, sd, feat = got.shape
    per = feat // LANES
    lane = lax.broadcasted_iota(jnp.int32, (HALF, LANES), 1) < HALF
    half = tmat_re.shape[1]
    planes[...] = jnp.zeros_like(planes)
    for g in range(ngrp):
        part = got[g]
        for q in range(per):
            t = g * per + q
            planes[pl.ds(t, sd, stride=PITCH), :] = part[:, q * LANES:(q + 1) * LANES].astype(F32)
    hi = maps[:LANES]
    lo = maps[LANES:]
    prods = []
    for s in range(0, sd, 2):
        pair = []
        for r in (s, s + 1):
            loc = planes[r * PITCH:r * PITCH + HALF, :]
            pair.append(jnp.concatenate([loc, swap_halves(loc)], axis=0).astype(BF16))
        both = jnp.concatenate(pair, axis=1)
        prod = dot(hi, both) + dot(lo, both)
        prods += [prod[:, :LANES], prod[:, LANES:]]
    for s in range(sd):
        prod = prods[s]
        field = near[s * HALF:(s + 1) * HALF, :] + jnp.where(lane, prod[:HALF], prod[HALF:])
        ur, ui = field[:half], field[half:2 * half]
        tr, ti = tmat_re[s], tmat_im[s]
        planes[s * PITCH:s * PITCH + half, :] = tr * ur - ti * ui
        planes[s * PITCH + half:s * PITCH + 2 * half, :] = tr * ui + ti * ur
    chunk = 2 * half // PARTS
    copies = []
    for t in range(2 * half):
        cols = slice(t * LANES, (t + 1) * LANES)
        ready[:, cols] = (x[:, cols].astype(F32) - planes[pl.ds(t, sd, stride=PITCH), :]).astype(BF16)
        if (t + 1) % chunk == 0:
            n = t // chunk
            span = pl.ds(n * chunk * LANES, chunk * LANES)
            copies.append(pltpu.make_async_copy(ready.at[:, span], out.at[:, span], sems.at[n]))
            copies[-1].start()
    for copy in copies:
        copy.wait()


def tail(got, near, coeffs, tmat_re, tmat_im, maps):
    sd = coeffs.shape[0]
    return pl.pallas_call(
        tail_kernel,
        out_shape=jax.ShapeDtypeStruct(coeffs.shape, BF16),
        out_specs=pl.BlockSpec(memory_space=pltpu.HBM),
        scratch_shapes=[
            pltpu.VMEM((sd * PITCH, LANES), F32),
            pltpu.VMEM(coeffs.shape, BF16),
            pltpu.SemaphoreType.DMA((PARTS,)),
        ],
        compiler_params=params(),
        name="tail",
    )(got, near, coeffs, tmat_re, tmat_im, maps)


def shards(coeffs, neighbours, counts, boxes, axial, rotations, out_map, coupling, in_map, tmat):
    sd, _ = coeffs.shape
    width = rotations.shape[1]
    ngrp = lax.axis_size("grp")
    ncell = lax.axis_size("cells")
    nbc = NBG * ngrp
    first = [p for i in range(0, ncell - 1, 2) for p in ((i, i + 1), (i + 1, i))]
    second = [p for i in range(1, ncell - 1, 2) for p in ((i, i + 1), (i + 1, i))]
    column = lax.axis_index("cells").astype(jnp.int32)[None]
    near_a = lax.ppermute(coeffs, "cells", first)
    near_b = lax.ppermute(coeffs, "cells", second)
    sent = pack(coeffs, boxes, ngrp)
    got = lax.all_to_all(sent, "grp", 0, 0, tiled=True)
    spot = jnp.arange(width, dtype=jnp.int32)
    spot = (spot % 2) * HALF + spot // 2
    lanes = jnp.arange(LANES, dtype=jnp.int32)
    perm = (spot[:, None] == lanes[None, :]).astype(BF16)
    permt = (lanes[:, None] == spot[None, :]).astype(BF16)
    turn, scale, maps, tre, tim = prepare(
        counts, axial, rotations, perm, permt, out_map, in_map, tmat
    )
    sums, onehot = box_sums(got, nbc, ncell)
    every = lax.all_to_all(sums, "cells", 0, 0, tiled=True)
    rows = sphere_rows(column, onehot, coupling)
    near = near_field(neighbours, column, near_a, coeffs, near_b, scale, turn)
    local = couple(rows, every, ngrp, sd)
    mine = lax.all_to_all(local, "grp", 0, 0, tiled=True)
    return tail(mine, near, coeffs, tre, tim, maps)


def solution(mesh):
    rows = P(("cells", "grp"), None)
    flat = P(("cells", "grp"))
    in_specs = (rows, rows, flat, flat, P(("cells", "grp"), None, None), P(), P(), P(), P(), rows)
    return jax.shard_map(shards, mesh=mesh, in_specs=in_specs, out_specs=rows, check_vma=False)
```
